256 devices in a mesh: row: 8 (over y, core), col: 32 (over z, x).
Axes of the slice: x: 4, y: 4, z: 8, core: 2. Of those that a mesh axis runs over, the one named last changes fastest.
Arguments:
- residuals: bfloat16 [131072, 32], P(('row', 'col')), may hold values from -6 to 6
- intersect_blocks: int32 [256, 4], P(('row', 'col')), may hold values from 0 to 3
- local_inverse: bfloat16 [131072, 1024], P(('row', 'col')), may hold values from -0.1875 to 0.1875
- coarse_basis: float32 [262144, 64], P(('row', 'col')), may hold values from -0.1875 to 0.1875
- coarse_slots: int32 [16384], replicated, may hold values from 0 to 16383, each once
- coarse_inverse: float32 [16384, 16384], P('row', 'col'), may hold values from -0.1875 to 0.1875
Outputs:
- preconditioned: float32 [131072, 32], P(('row', 'col'))
The draws below stay inside these ranges and needn't reach their ends.
Inputs may be any that keep to these rules, and one draw needn't show every extreme that they name: `intersect_blocks`: each entry names one of the four owned blocks. `coarse_slots`: every coarse index from 0 to 16383 appears exactly once.
All inputs are finite; a program needn't handle non-finite values.
Results may differ from the reference program's by a relative error of at most 0.0003.
Values may be sent and summed in bfloat16 or wider, within the bound.
A program may use at most 64 MiB of HBM per device.

```python
import jax
import jax.numpy as jnp
from jax import lax

BLK = 128
OWN = 512
LOC = 1024
RHS = 32
NEV = 64
COARSE = 16384
DOFS = 131072
N_ROW = 8
N_COL = 32
DEVICES = 256


def set_ends(array, rng, smallest, largest):
    shape = array.shape
    spot = [jax.random.randint(jax.random.fold_in(rng, axis), (), 0, shape[axis]) for axis in range(len(shape))]
    array = array.at[tuple(spot)].set(smallest)
    longest = shape.index(max(shape))
    spot[longest] = (spot[longest] + 1) % shape[longest]
    return array.at[tuple(spot)].set(largest)


def shard_levels(own_key, extent, shards, smallest, high):
    loudness = 1.0
    for position, parts in shards:
        steps = jax.random.uniform(jax.random.fold_in(jax.random.fold_in(own_key, 6), position), (parts,), jnp.float32, smallest / len(shards), high / len(shards))
        loudness = loudness * jnp.repeat(jnp.exp(steps), extent[position] // parts).reshape((-1,) + (1,) * (len(extent) - 1 - position))
    return loudness


def bell_draw(own_key, shape, scale, bound, split=(), kind=jnp.bfloat16):
    array = jax.random.normal(own_key, shape, jnp.float32) * scale
    if len(split) > 0:
        array = shard_levels(own_key, shape, split, -0.22, 0.18) * array
    return jnp.clip(array, min=-bound, max=bound).astype(kind)


def setup_inputs(seed: int = 0) -> dict:
    keys = jax.random.split(jax.random.key(seed), 7)
    return {
        "residuals": bell_draw(keys[0], (DOFS, RHS), 1.0, 6.0, ((0, 256),)),
        "intersect_blocks": set_ends(jax.random.randint(keys[1], (DEVICES, 4), 0, 4), jax.random.fold_in(keys[1], 1), 0, 3).astype(jnp.int32),
        "local_inverse": bell_draw(keys[2], (DOFS, LOC), LOC ** -0.5, 0.1875, ((0, 256),)),
        "coarse_basis": bell_draw(keys[3], (DEVICES * LOC, NEV), LOC ** -0.5, 0.1875, ((0, 256),), jnp.float32),
        "coarse_slots": jax.random.permutation(keys[4], COARSE).astype(jnp.int32),
        "coarse_inverse": bell_draw(keys[5], (COARSE, COARSE), (COARSE // 16) ** -0.5, 0.1875, ((0, 8), (1, 32)), jnp.float32),
    }


def shift_grid(field, axis, by):
    count = field.shape[axis]
    moved = jnp.roll(field, by, axis=axis)
    source = jnp.arange(count, dtype=jnp.int32) - by
    valid = ((source >= 0) & (source < count)).astype(field.dtype)
    shape = [1] * field.ndim
    shape[axis] = count
    return moved * valid.reshape(shape)


def local_product(pair):
    return jnp.dot(pair[0], pair[1], preferred_element_type=jnp.float32)


def reference(residuals, intersect_blocks, local_inverse, coarse_basis, coarse_slots, coarse_inverse):
    nrows = N_ROW
    ncols = N_COL
    blocks = residuals.reshape(nrows, ncols, OWN // BLK, BLK, RHS)
    sends = intersect_blocks.reshape(nrows, ncols, 4).astype(jnp.int32)
    outgoing = jnp.take_along_axis(blocks, sends[:, :, :, None, None], axis=2)
    incoming = jnp.stack([shift_grid(outgoing[:, :, 0], 0, 1), shift_grid(outgoing[:, :, 1], 0, -1),
                          shift_grid(outgoing[:, :, 2], 1, 1), shift_grid(outgoing[:, :, 3], 1, -1)], axis=2)
    local_vec = jnp.concatenate([residuals.reshape(nrows, ncols, OWN, RHS),
                                 incoming.reshape(nrows, ncols, LOC - OWN, RHS)], axis=2).reshape(DEVICES, LOC, RHS)
    inverse = local_inverse.reshape(DEVICES, OWN, LOC)
    schwarz = lax.map(local_product, (inverse, local_vec))
    basis = coarse_basis.reshape(DEVICES, LOC, NEV)
    partial_value = jnp.einsum("dln,dlr->dnr", basis, local_vec.astype(jnp.float32), precision=lax.Precision.HIGHEST)
    coarse_rhs = jnp.zeros((COARSE, RHS), jnp.float32).at[coarse_slots].set(partial_value.reshape(COARSE, RHS))
    coarse_sol = jnp.dot(coarse_inverse, coarse_rhs, precision=lax.Precision.HIGHEST)
    own_coarse = coarse_sol[coarse_slots].reshape(DEVICES, NEV, RHS)
    prolonged = jnp.einsum("dln,dnr->dlr", basis, own_coarse, precision=lax.Precision.HIGHEST)
    grid = prolonged.reshape(nrows, ncols, LOC, RHS)
    returning = grid[:, :, OWN:].reshape(nrows, ncols, 4, BLK, RHS)
    returned = jnp.stack([shift_grid(returning[:, :, 0], 0, -1), shift_grid(returning[:, :, 1], 0, 1),
                          shift_grid(returning[:, :, 2], 1, -1), shift_grid(returning[:, :, 3], 1, 1)], axis=2)
    matches = (sends[..., None] == jnp.arange(OWN // BLK, dtype=jnp.int32)).astype(jnp.float32)
    added = jnp.einsum("rcdb,rcdkq->rcbkq", matches, returned, precision=lax.Precision.HIGHEST)
    result = schwarz.reshape(nrows, ncols, OWN, RHS) + grid[:, :, :OWN] + added.reshape(nrows, ncols, OWN, RHS)
    return result.reshape(DOFS, RHS)
```

```python
import functools

import jax
import jax.numpy as jnp
from jax import lax
from jax.experimental import pallas as pl
from jax.experimental.pallas import tpu as pltpu
from jax.sharding import PartitionSpec as P

MESH = pl.DeviceIdType.MESH
BLK = 128
LANES = 128
NX = 4
CORES = 2
NT = (((1,), (1,)), ((), ()))
NN = (((1,), (0,)), ((), ()))
F32 = jnp.float32
BF16 = jnp.bfloat16


def matmul(a, b, dims):
    return lax.dot_general(a, b, dims, preferred_element_type=F32)


def split(x):
    hi = x.astype(BF16)
    return hi, (x - hi.astype(F32)).astype(BF16)


def lane_low(shape):
    return lax.broadcasted_iota(jnp.int32, shape, len(shape) - 1) < LANES // 2


def half_roll(x):
    return pltpu.roll(x, LANES // 2, 1)


def far_first(count):
    return sorted(range(1, count), key=lambda k: -min(k, count - k))


def tree_sum(parts):
    while len(parts) > 1:
        parts = [parts[i] + parts[i + 1] if i + 1 < len(parts) else parts[i] for i in range(0, len(parts), 2)]
    return parts[0]


def kernel(
    nrow,
    ncol,
    res_hbm,
    ib_hbm,
    linv_hbm,
    basis_hbm,
    slots_hbm,
    coarse_hbm,
    out_ref,
    res_ref,
    ib_ref,
    slots_ref,
    outgoing,
    incoming,
    linv,
    basis,
    basis2,
    coarse,
    coarse_hi,
    coarse_lo,
    hot_in,
    hot_out,
    plane1,
    cross1,
    line1,
    rhs_all,
    pieces,
    received,
    plane2,
    cross2,
    line2,
    picks,
    lent,
    wide_hi,
    wide_lo,
    load_sem,
    halo_send,
    halo_recv,
    lend_send,
    lend_recv,
    pick_send,
    pick_recv,
    bulk_send,
    bulk_recv,
):
    r = lax.axis_index("row")
    c = lax.axis_index("col")
    z, x = c // NX, lax.rem(c, NX)
    y, core = r // CORES, lax.rem(r, CORES)
    nz, ny = ncol // NX, nrow // CORES
    nplane = nrow * NX
    rhs = res_ref.shape[0]
    own = res_ref.shape[1]
    half = rhs // 2
    rows, width = coarse.shape
    nev = basis.shape[0]
    low = lane_low((half, LANES))
    mine = r * NX + x

    def row_at(dy, dk):
        return lax.rem(y + dy, ny) * CORES + lax.rem(core + dk, CORES)

    plane_offsets = sorted(
        ((dx, dy, dk) for dx in range(NX) for dy in range(ny) for dk in range(CORES) if (dx, dy, dk) != (0, 0, 0)),
        key=lambda o: -(min(o[0], NX - o[0]) + min(o[1], ny - o[1]) + 0.5 * o[2]))
    row_offsets = [(dy, dk) for dx, dy, dk in plane_offsets if dx == 0]

    def plane_peer(dx, dy, dk):
        return (row_at(dy, dk), z * NX + lax.rem(x + dx, NX))

    def line_peer(dz):
        return (r, lax.rem(z + dz, nz) * NX + x)

    exists = [r < nrow - 1, r > 0, c < ncol - 1, c > 0]
    target = [(r + 1, c), (r - 1, c), (r, c + 1), (r, c - 1)]
    opposite = [1, 0, 3, 2]
    up = jnp.logical_and(x == NX - 1, exists[2])
    down = jnp.logical_and(x == 0, exists[3])

    barrier = pltpu.get_barrier_semaphore()

    def greet(device):
        pl.semaphore_signal(barrier, inc=1, device_id=device, device_id_type=MESH)

    for offset in plane_offsets:
        greet(plane_peer(*offset))
    for dz in far_first(nz):
        greet(line_peer(dz))

    @pl.when(up)
    def _():
        greet(target[2])

    @pl.when(down)
    def _():
        greet(target[3])

    loads = [
        pltpu.make_async_copy(basis_hbm, basis, load_sem.at[0]),
        pltpu.make_async_copy(coarse_hbm, coarse, load_sem.at[1]),
        pltpu.make_async_copy(linv_hbm, linv, load_sem.at[2]),
        pltpu.make_async_copy(res_hbm, res_ref, load_sem.at[3]),
        pltpu.make_async_copy(ib_hbm, ib_ref, load_sem.at[4]),
        pltpu.make_async_copy(slots_hbm, slots_ref, load_sem.at[5]),
    ]
    for i in (3, 4, 0, 5, 1, 2):
        loads[i].start()
    loads[4].wait()
    loads[3].wait()

    blocks = [res_ref[:, b * BLK:(b + 1) * BLK] for b in range(own // BLK)]
    for d in range(4):
        index = ib_ref[0, d]
        value = blocks[0]
        for b in range(1, len(blocks)):
            value = jnp.where(index == b, blocks[b], value)
        outgoing[d] = value

        @pl.when(jnp.logical_not(exists[opposite[d]]))
        def _():
            incoming[d] = jnp.zeros_like(incoming[d])

        @pl.when(jnp.logical_not(exists[d]))
        def _():
            lent[d] = jnp.zeros_like(lent[d])
            picks[1 + d] = jnp.zeros_like(picks[1 + d])

    picks[5] = jnp.zeros_like(picks[5])

    def halo(d):
        return pltpu.make_async_remote_copy(
            src_ref=outgoing.at[d], dst_ref=incoming.at[d],
            send_sem=halo_send.at[d], recv_sem=halo_recv.at[d],
            device_id=target[d], device_id_type=MESH)

    def lend(d):
        return pltpu.make_async_remote_copy(
            src_ref=basis.at[:, pl.ds(own + d * BLK, BLK)], dst_ref=lent.at[d],
            send_sem=lend_send.at[d], recv_sem=lend_recv.at[d],
            device_id=target[opposite[d]], device_id_type=MESH)

    def pick(d):
        return pltpu.make_async_remote_copy(
            src_ref=picks.at[0], dst_ref=picks.at[1 + d],
            send_sem=pick_send.at[d], recv_sem=pick_recv.at[d],
            device_id=target[opposite[d]], device_id_type=MESH)

    def send(phase, src, dst, device):
        pltpu.make_async_remote_copy(
            src_ref=src, dst_ref=dst, send_sem=bulk_send.at[phase], recv_sem=bulk_recv.at[phase],
            device_id=device, device_id_type=MESH).start()

    def arrived(phase, buf, count):
        some = buf.at[pl.ds(0, count)]
        pltpu.make_async_copy(some, some, bulk_recv.at[phase]).wait()

    def drained(phase, buf, count):
        some = buf.at[pl.ds(0, count)]
        pltpu.make_async_copy(some, some, bulk_send.at[phase]).wait()

    def spread_plane(phase, buf):
        for offset in plane_offsets:
            send(phase, buf.at[mine], buf.at[mine], plane_peer(*offset))

    def exchange_line(phase, src, dst):
        for dz in far_first(nz):
            to = lax.rem(z + dz, nz)
            send(phase, src.at[to], dst.at[z], (r, to * NX + x))

    def unpacked(buf, count):
        tops, bots = [], []
        for p in range(count // 2):
            a, b = buf[2 * p], buf[2 * p + 1]
            tops.append(jnp.where(low, a, half_roll(b)))
            bots.append(jnp.where(low, half_roll(a), b))
        value = jnp.concatenate([jnp.concatenate(tops, axis=1), jnp.concatenate(bots, axis=1)], axis=0)
        return jnp.concatenate(split(value), axis=0)

    def packed(part, put):
        for q in range(part.shape[1] // LANES):
            top = part[:half, q * LANES:(q + 1) * LANES]
            bot = part[half:, q * LANES:(q + 1) * LANES]
            put(2 * q, jnp.where(low, top, half_roll(bot)))
            put(2 * q + 1, jnp.where(low, half_roll(top), bot))

    plane_width = NX * nev
    share = width // nrow
    loads[5].wait()
    place_in = lax.broadcasted_iota(jnp.int32, (share, plane_width), 0)

    def build_in(i, carry):
        start = pl.multiple_of(i * (ncol * nev) + z * plane_width, plane_width)
        slot = slots_ref[:, pl.ds(start, plane_width)] - (x * width + r * share)
        at = pl.ds(pl.multiple_of(i * plane_width, plane_width), plane_width)
        for t in range(nz):
            hot = jnp.where(place_in == slot - t * (NX * width), 1.0, 0.0)
            hot_in[t * share:(t + 1) * share, at] = hot.astype(BF16)
        return carry

    lax.fori_loop(0, nrow, build_in, 0)

    loads[0].wait()
    b_hi, b_lo = split(basis[...])
    basis2[:nev] = b_hi
    basis2[nev:] = b_lo
    partial = matmul(res_ref[...], basis2[:, :own], NT)

    extra = up.astype(jnp.int32) + down.astype(jnp.int32)
    pl.semaphore_wait(barrier, nplane - 1 + nz - 1 + extra)
    for d in range(4):
        @pl.when(exists[d])
        def _():
            halo(d).start()
    for d in range(4):
        @pl.when(exists[opposite[d]])
        def _():
            lend(d).start()

    loads[1].wait()
    a_hi, a_lo = split(coarse[...])
    coarse_hi[...] = a_hi
    coarse_lo[...] = a_lo

    for d in range(4):
        @pl.when(exists[opposite[d]])
        def _():
            halo(d).wait_recv()

    inc = jnp.concatenate([incoming[d] for d in range(4)], axis=1)
    partial = partial + matmul(inc, basis2[:, own:], NT)
    partial = partial + half_roll(partial)
    plane1[mine] = jnp.where(low, partial[:half], partial[half:])
    spread_plane(0, plane1)

    loads[2].wait()
    local = jnp.concatenate([res_ref[...], inc], axis=1)
    out_ref[...] = matmul(local, linv[...], NT)

    low8 = lane_low((8, LANES))
    wanted = []
    for t in range(nz // 2):
        pair = []
        for device in (r * ncol + 2 * t * NX + x, r * ncol + (2 * t + 1) * NX + x):
            at = pl.ds(pl.multiple_of((device // 2) * LANES, LANES), LANES)
            pair.append(jnp.broadcast_to(slots_ref[:, at], (8, LANES)))
        even = jnp.where(low8, pair[0], half_roll(pair[1]))
        odd = jnp.where(low8, half_roll(pair[0]), pair[1])
        wanted.append(jnp.where(lax.rem(x, 2) == 0, even, odd)[:1])
    wanted = jnp.concatenate(wanted, axis=1)
    place_out = lax.broadcasted_iota(jnp.int32, (plane_width, nz * nev), 0)

    def build_out(i, carry):
        at = pl.ds(pl.multiple_of(i * plane_width, plane_width), plane_width)
        hot = jnp.where(place_out == wanted - (i * rows + z * plane_width), 1.0, 0.0)
        hot_out[at] = hot.astype(BF16)
        return carry

    lax.fori_loop(0, nrow, build_out, 0)

    wide_hi[:nev] = basis2[:nev, :own]
    wide_lo[:nev] = basis2[nev:, :own]
    wide_hi[5 * nev:] = jnp.zeros_like(wide_hi[5 * nev:])
    wide_lo[5 * nev:] = jnp.zeros_like(wide_lo[5 * nev:])
    for d in range(4):
        @pl.when(exists[d])
        def _():
            lend(d).wait_recv()

        l_hi, l_lo = split(lent[d])
        for b in range(own // BLK):
            here = ib_ref[0, d] == b
            at = slice((d + 1) * nev, (d + 2) * nev), slice(b * BLK, (b + 1) * BLK)
            wide_hi[at] = jnp.where(here, l_hi, jnp.zeros_like(l_hi))
            wide_lo[at] = jnp.where(here, l_lo, jnp.zeros_like(l_lo))

    def select(phase, plane, hot, dims, cross, line):
        arrived(phase, plane, nplane - 1)
        part = matmul(unpacked(plane, nplane), hot[...], dims)
        part = part[:rhs] + part[rhs:]

        def put(i, value):
            cross[i] = value

        packed(part, put)
        exchange_line(phase + 1, cross, line)
        line[z] = cross[z]
        arrived(phase + 1, line, nz - 1)
        return tree_sum([line[i] for i in range(nz)])

    rhs_all[r] = select(0, plane1, hot_in, NT, cross1, line1)
    for dy, dk in row_offsets:
        send(2, rhs_all.at[r], rhs_all.at[r], (row_at(dy, dk), c))
    arrived(2, rhs_all, nrow - 1)
    column2 = unpacked(rhs_all, nrow)

    span = rows // nz
    for dz in far_first(nz) + [0]:
        block = lax.rem(z + dz, nz)
        at = pl.ds(pl.multiple_of(block * span, span), span)
        part = matmul(column2, coarse_hi[at], NT) + matmul(column2, coarse_lo[at], NT)

        def put(i, value):
            pieces[block * NX + i] = value

        packed(part[:rhs] + part[rhs:], put)
        for dx in (2, 1, 3, 0) if dz else (2, 1, 3):
            to = block * NX + lax.rem(x + dx, NX)
            send(3, pieces.at[to], received.at[c], (r, to))

    received[c] = pieces[c]
    arrived(3, received, ncol - 1)
    plane2[mine] = tree_sum([received[i] for i in range(ncol)])

    spread_plane(4, plane2)
    picks[0] = select(4, plane2, hot_out, NN, cross2, line2)
    for d in range(4):
        @pl.when(exists[opposite[d]])
        def _():
            pick(d).start()
    for d in range(4):
        @pl.when(exists[d])
        def _():
            pick(d).wait_recv()

    picked = unpacked(picks, 6)
    inner = matmul(picked, wide_hi[...], NN) + matmul(picked, wide_lo[...], NN)
    out_ref[...] = out_ref[...] + inner[:rhs] + inner[rhs:]

    drained(0, plane1, nplane - 1)
    drained(1, line1, nz - 1)
    drained(2, rhs_all, nrow - 1)
    drained(3, received, ncol - 1)
    drained(4, plane2, nplane - 1)
    drained(5, line2, nz - 1)
    for d in range(4):
        @pl.when(exists[d])
        def _():
            halo(d).wait_send()

        @pl.when(exists[opposite[d]])
        def _():
            lend(d).wait_send()
            pick(d).wait_send()


def shards(nrow, ncol, residuals, intersect_blocks, local_inverse, coarse_basis, coarse_slots, coarse_inverse):
    own, rhs = residuals.shape
    loc, nev = coarse_basis.shape
    rows, width = coarse_inverse.shape
    total = coarse_slots.shape[0]
    nz = ncol // NX
    nplane = nrow * NX
    assert 2 * nev == LANES and rows == ncol * nev and width == nrow * nev and loc == own + 4 * BLK and own % BLK == 0
    packed = (rhs // 2, LANES)
    vmem = pl.BlockSpec(memory_space=pltpu.VMEM)
    hbm = pl.BlockSpec(memory_space=pl.ANY)
    dma = pltpu.SemaphoreType.DMA
    out = pl.pallas_call(
        functools.partial(kernel, nrow, ncol),
        name="schwarz",
        out_shape=pltpu.VMEM((rhs, own), F32),
        in_specs=[hbm] * 6,
        out_specs=vmem,
        scratch_shapes=[
            pltpu.VMEM((rhs, own), BF16),
            pltpu.SMEM(intersect_blocks.shape, jnp.int32),
            pltpu.VMEM((1, total), jnp.int32),
            pltpu.VMEM((4, rhs, BLK), BF16),
            pltpu.VMEM((4, rhs, BLK), BF16),
            pltpu.VMEM((own, loc), BF16),
            pltpu.VMEM((nev, loc), F32),
            pltpu.VMEM((2 * nev, loc), BF16),
            pltpu.VMEM((rows, width), F32),
            pltpu.VMEM((rows, width), BF16),
            pltpu.VMEM((rows, width), BF16),
            pltpu.VMEM((nz * nev, nplane * nev), BF16),
            pltpu.VMEM((nplane * nev, nz * nev), BF16),
            pltpu.VMEM((nplane,) + packed, F32),
            pltpu.VMEM((nz,) + packed, F32),
            pltpu.VMEM((nz,) + packed, F32),
            pltpu.VMEM((nrow,) + packed, F32),
            pltpu.VMEM((ncol,) + packed, F32),
            pltpu.VMEM((ncol,) + packed, F32),
            pltpu.VMEM((nplane,) + packed, F32),
            pltpu.VMEM((nz,) + packed, F32),
            pltpu.VMEM((nz,) + packed, F32),
            pltpu.VMEM((6,) + packed, F32),
            pltpu.VMEM((4, nev, BLK), F32),
            pltpu.VMEM((6 * nev, own), BF16),
            pltpu.VMEM((6 * nev, own), BF16),
            dma((6,)),
            dma((4,)),
            dma((4,)),
            dma((4,)),
            dma((4,)),
            dma((4,)),
            dma((4,)),
            dma((6,)),
            dma((6,)),
        ],
        compiler_params=pltpu.CompilerParams(collective_id=0, has_side_effects=True),
    )(
        residuals.T,
        intersect_blocks,
        local_inverse,
        coarse_basis.T,
        coarse_slots.reshape(1, total),
        coarse_inverse,
    )
    return out.T


def solution(mesh):
    placed = (
        P(("row", "col"), None),
        P(("row", "col"), None),
        P(("row", "col"), None),
        P(("row", "col"), None),
        P(),
        P("row", "col"),
    )
    return jax.shard_map(
        functools.partial(shards, mesh.shape["row"], mesh.shape["col"]),
        mesh=mesh, in_specs=placed, out_specs=P(("row", "col"), None), check_vma=False,
    )
```

```python
import functools

import jax
import jax.numpy as jnp
from jax import lax
from jax.experimental import pallas as pl
from jax.experimental.pallas import tpu as pltpu
from jax.sharding import PartitionSpec as P

MESH = pl.DeviceIdType.MESH
BLK = 128
LANES = 128
NX = 4
CORES = 2
NT = (((1,), (1,)), ((), ()))
NN = (((1,), (0,)), ((), ()))
F32 = jnp.float32
BF16 = jnp.bfloat16


def matmul(a, b, dims):
    return lax.dot_general(a, b, dims, preferred_element_type=F32)


def split(x):
    hi = x.astype(BF16)
    return hi, (x - hi.astype(F32)).astype(BF16)


def lane_low(shape):
    return lax.broadcasted_iota(jnp.int32, shape, len(shape) - 1) < LANES // 2


def half_roll(x):
    return pltpu.roll(x, LANES // 2, 1)


def far_first(count):
    return sorted(range(1, count), key=lambda k: -min(k, count - k))


def tree_sum(parts):
    while len(parts) > 1:
        parts = [parts[i] + parts[i + 1] if i + 1 < len(parts) else parts[i] for i in range(0, len(parts), 2)]
    return parts[0]


def kernel(
    nrow,
    ncol,
    res_hbm,
    ib_hbm,
    linv_hbm,
    basis_hbm,
    slots_hbm,
    coarse_hbm,
    out_ref,
    res_ref,
    ib_ref,
    slots_ref,
    outgoing,
    incoming,
    linv,
    basis,
    basis2,
    coarse,
    coarse_t,
    hot_in,
    hot_out,
    plane1,
    cross1,
    line1,
    rhs_all,
    pieces,
    received,
    plane2,
    cross2,
    line2,
    picks,
    lent,
    wide_hi,
    wide_lo,
    load_sem,
    halo_send,
    halo_recv,
    lend_send,
    lend_recv,
    pick_send,
    pick_recv,
    bulk_send,
    bulk_recv,
):
    r = lax.axis_index("row")
    c = lax.axis_index("col")
    z, x = c // NX, lax.rem(c, NX)
    y, core = r // CORES, lax.rem(r, CORES)
    nz, ny = ncol // NX, nrow // CORES
    nplane = nrow * NX
    rhs = res_ref.shape[0]
    own = res_ref.shape[1]
    half = rhs // 2
    rows, width = coarse.shape
    nev = basis.shape[0]
    low = lane_low((half, LANES))
    mine = r * NX + x

    def row_at(dy, dk):
        return lax.rem(y + dy, ny) * CORES + lax.rem(core + dk, CORES)

    plane_offsets = sorted(
        ((dx, dy, dk) for dx in range(NX) for dy in range(ny) for dk in range(CORES) if (dx, dy, dk) != (0, 0, 0)),
        key=lambda o: -(min(o[0], NX - o[0]) + min(o[1], ny - o[1]) + 0.5 * o[2]))
    row_offsets = [(dy, dk) for dx, dy, dk in plane_offsets if dx == 0]

    def plane_peer(dx, dy, dk):
        return (row_at(dy, dk), z * NX + lax.rem(x + dx, NX))

    def line_peer(dz):
        return (r, lax.rem(z + dz, nz) * NX + x)

    exists = [r < nrow - 1, r > 0, c < ncol - 1, c > 0]
    target = [(r + 1, c), (r - 1, c), (r, c + 1), (r, c - 1)]
    opposite = [1, 0, 3, 2]
    up = jnp.logical_and(x == NX - 1, exists[2])
    down = jnp.logical_and(x == 0, exists[3])

    barrier = pltpu.get_barrier_semaphore()

    def greet(device):
        pl.semaphore_signal(barrier, inc=1, device_id=device, device_id_type=MESH)

    for offset in plane_offsets:
        greet(plane_peer(*offset))
    for dz in far_first(nz):
        greet(line_peer(dz))

    @pl.when(up)
    def _():
        greet(target[2])

    @pl.when(down)
    def _():
        greet(target[3])

    loads = [
        pltpu.make_async_copy(basis_hbm, basis, load_sem.at[0]),
        pltpu.make_async_copy(coarse_hbm, coarse, load_sem.at[1]),
        pltpu.make_async_copy(linv_hbm, linv, load_sem.at[2]),
        pltpu.make_async_copy(res_hbm, res_ref, load_sem.at[3]),
        pltpu.make_async_copy(ib_hbm, ib_ref, load_sem.at[4]),
        pltpu.make_async_copy(slots_hbm, slots_ref, load_sem.at[5]),
    ]
    for i in (3, 4, 0, 5, 1, 2):
        loads[i].start()
    loads[4].wait()
    loads[3].wait()

    blocks = [res_ref[:, b * BLK:(b + 1) * BLK] for b in range(own // BLK)]
    for d in range(4):
        index = ib_ref[0, d]
        value = blocks[0]
        for b in range(1, len(blocks)):
            value = jnp.where(index == b, blocks[b], value)
        outgoing[d] = value

        @pl.when(jnp.logical_not(exists[opposite[d]]))
        def _():
            incoming[d] = jnp.zeros_like(incoming[d])

        @pl.when(jnp.logical_not(exists[d]))
        def _():
            lent[d] = jnp.zeros_like(lent[d])
            picks[1 + d] = jnp.zeros_like(picks[1 + d])

    picks[5] = jnp.zeros_like(picks[5])

    def halo(d):
        return pltpu.make_async_remote_copy(
            src_ref=outgoing.at[d], dst_ref=incoming.at[d],
            send_sem=halo_send.at[d], recv_sem=halo_recv.at[d],
            device_id=target[d], device_id_type=MESH)

    def lend(d):
        return pltpu.make_async_remote_copy(
            src_ref=basis.at[:, pl.ds(own + d * BLK, BLK)], dst_ref=lent.at[d],
            send_sem=lend_send.at[d], recv_sem=lend_recv.at[d],
            device_id=target[opposite[d]], device_id_type=MESH)

    def pick(d):
        return pltpu.make_async_remote_copy(
            src_ref=picks.at[0], dst_ref=picks.at[1 + d],
            send_sem=pick_send.at[d], recv_sem=pick_recv.at[d],
            device_id=target[opposite[d]], device_id_type=MESH)

    def send(phase, src, dst, device):
        pltpu.make_async_remote_copy(
            src_ref=src, dst_ref=dst, send_sem=bulk_send.at[phase], recv_sem=bulk_recv.at[phase],
            device_id=device, device_id_type=MESH).start()

    def arrived(phase, buf, count):
        some = buf.at[pl.ds(0, count)]
        pltpu.make_async_copy(some, some, bulk_recv.at[phase]).wait()

    def drained(phase, buf, count):
        some = buf.at[pl.ds(0, count)]
        pltpu.make_async_copy(some, some, bulk_send.at[phase]).wait()

    def spread_plane(phase, buf):
        for offset in plane_offsets:
            send(phase, buf.at[mine], buf.at[mine], plane_peer(*offset))

    def exchange_line(phase, src, dst):
        for dz in far_first(nz):
            to = lax.rem(z + dz, nz)
            send(phase, src.at[to], dst.at[z], (r, to * NX + x))

    def unpacked(buf, count):
        tops, bots = [], []
        for p in range(count // 2):
            a, b = buf[2 * p], buf[2 * p + 1]
            tops.append(jnp.where(low, a, half_roll(b)))
            bots.append(jnp.where(low, half_roll(a), b))
        value = jnp.concatenate([jnp.concatenate(tops, axis=1), jnp.concatenate(bots, axis=1)], axis=0)
        return jnp.concatenate(split(value), axis=0)

    def packed(part, put):
        for q in range(part.shape[1] // LANES):
            top = part[:half, q * LANES:(q + 1) * LANES]
            bot = part[half:, q * LANES:(q + 1) * LANES]
            put(2 * q, jnp.where(low, top, half_roll(bot)))
            put(2 * q + 1, jnp.where(low, half_roll(top), bot))

    extra = up.astype(jnp.int32) + down.astype(jnp.int32)
    pl.semaphore_wait(barrier, nplane - 1 + nz - 1 + extra)
    for d in range(4):
        @pl.when(exists[d])
        def _():
            halo(d).start()

    plane_width = NX * nev
    share = width // nrow
    loads[5].wait()
    place_in = lax.broadcasted_iota(jnp.int32, (share, plane_width), 0)

    def build_in(i, carry):
        start = pl.multiple_of(i * (ncol * nev) + z * plane_width, plane_width)
        slot = slots_ref[:, pl.ds(start, plane_width)] - (x * width + r * share)
        at = pl.ds(pl.multiple_of(i * plane_width, plane_width), plane_width)
        for t in range(nz):
            hot = jnp.where(place_in == slot - t * (NX * width), 1.0, 0.0)
            hot_in[t * share:(t + 1) * share, at] = hot.astype(BF16)
        return carry

    lax.fori_loop(0, nrow, build_in, 0)

    loads[0].wait()
    b_hi, b_lo = split(basis[...])
    basis2[:nev] = b_hi
    basis2[nev:] = b_lo
    partial = matmul(res_ref[...], basis2[:, :own], NT)

    for d in range(4):
        @pl.when(exists[opposite[d]])
        def _():
            halo(d).wait_recv()

    inc = jnp.concatenate([incoming[d] for d in range(4)], axis=1)
    partial = partial + matmul(inc, basis2[:, own:], NT)
    partial = partial + half_roll(partial)
    plane1[mine] = jnp.where(low, partial[:half], partial[half:])
    spread_plane(0, plane1)

    span = rows // nz
    loads[1].wait()
    for t in range(nz):
        at = slice(t * span, (t + 1) * span)
        coarse_t[:width, at], coarse_t[width:, at] = split(coarse[at].T)

    loads[2].wait()
    local = jnp.concatenate([res_ref[...], inc], axis=1)
    out_ref[...] = matmul(local, linv[...], NT)

    low8 = lane_low((8, LANES))
    wanted = []
    for t in range(nz // 2):
        pair = []
        for device in (r * ncol + 2 * t * NX + x, r * ncol + (2 * t + 1) * NX + x):
            at = pl.ds(pl.multiple_of((device // 2) * LANES, LANES), LANES)
            pair.append(jnp.broadcast_to(slots_ref[:, at], (8, LANES)))
        even = jnp.where(low8, pair[0], half_roll(pair[1]))
        odd = jnp.where(low8, half_roll(pair[0]), pair[1])
        wanted.append(jnp.where(lax.rem(x, 2) == 0, even, odd)[:1])
    wanted = jnp.concatenate(wanted, axis=1)
    place_out = lax.broadcasted_iota(jnp.int32, (plane_width, nz * nev), 0)

    def build_out(i, carry):
        at = pl.ds(pl.multiple_of(i * plane_width, plane_width), plane_width)
        hot = jnp.where(place_out == wanted - (i * rows + z * plane_width), 1.0, 0.0)
        hot_out[at] = hot.astype(BF16)
        return carry

    lax.fori_loop(0, nrow, build_out, 0)

    def select(phase, plane, hot, dims, cross, line, meanwhile):
        arrived(phase, plane, nplane - 1)
        part = matmul(unpacked(plane, nplane), hot[...], dims)
        part = part[:rhs] + part[rhs:]

        def put(i, value):
            cross[i] = value

        packed(part, put)
        exchange_line(phase + 1, cross, line)
        line[z] = cross[z]
        meanwhile()
        arrived(phase + 1, line, nz - 1)
        return tree_sum([line[i] for i in range(nz)])

    def lend_all():
        for d in range(4):
            @pl.when(exists[opposite[d]])
            def _():
                lend(d).start()

    rhs_all[r] = select(0, plane1, hot_in, NT, cross1, line1, lend_all)
    for dy, dk in row_offsets:
        send(2, rhs_all.at[r], rhs_all.at[r], (row_at(dy, dk), c))
    arrived(2, rhs_all, nrow - 1)
    column2 = unpacked(rhs_all, nrow)

    column4 = jnp.concatenate([column2, column2], axis=1)
    steps = far_first(nz) + [0]
    for batch in (steps[:nz // 2], steps[nz // 2:]):
        parts = []
        for dz in batch:
            block = lax.rem(z + dz, nz)
            at = pl.ds(pl.multiple_of(block * span, span), span)
            parts.append((block, matmul(column4, coarse_t[:, at], NN)))
        for block, part in parts:
            def put(i, value):
                pieces[block * NX + i] = value

            packed(part[:rhs] + part[rhs:], put)
        for dz, (block, part) in zip(batch, parts):
            for dx in (2, 1, 3, 0) if dz else (2, 1, 3):
                to = block * NX + lax.rem(x + dx, NX)
                send(3, pieces.at[to], received.at[c], (r, to))

    wide_hi[:nev] = basis2[:nev, :own]
    wide_lo[:nev] = basis2[nev:, :own]
    wide_hi[5 * nev:] = jnp.zeros_like(wide_hi[5 * nev:])
    wide_lo[5 * nev:] = jnp.zeros_like(wide_lo[5 * nev:])
    for d in range(4):
        @pl.when(exists[d])
        def _():
            lend(d).wait_recv()

        l_hi, l_lo = split(lent[d])
        for b in range(own // BLK):
            here = ib_ref[0, d] == b
            at = slice((d + 1) * nev, (d + 2) * nev), slice(b * BLK, (b + 1) * BLK)
            wide_hi[at] = jnp.where(here, l_hi, jnp.zeros_like(l_hi))
            wide_lo[at] = jnp.where(here, l_lo, jnp.zeros_like(l_lo))

    received[c] = pieces[c]
    arrived(3, received, ncol - 1)
    plane2[mine] = tree_sum([received[i] for i in range(ncol)])

    spread_plane(4, plane2)
    picks[0] = select(4, plane2, hot_out, NN, cross2, line2, lambda: None)
    for d in range(4):
        @pl.when(exists[opposite[d]])
        def _():
            pick(d).start()
    for d in range(4):
        @pl.when(exists[d])
        def _():
            pick(d).wait_recv()

    picked = unpacked(picks, 6)
    inner = matmul(picked, wide_hi[...], NN) + matmul(picked, wide_lo[...], NN)
    out_ref[...] = out_ref[...] + inner[:rhs] + inner[rhs:]

    drained(0, plane1, nplane - 1)
    drained(1, line1, nz - 1)
    drained(2, rhs_all, nrow - 1)
    drained(3, received, ncol - 1)
    drained(4, plane2, nplane - 1)
    drained(5, line2, nz - 1)
    for d in range(4):
        @pl.when(exists[d])
        def _():
            halo(d).wait_send()

        @pl.when(exists[opposite[d]])
        def _():
            lend(d).wait_send()
            pick(d).wait_send()


def shards(nrow, ncol, residuals, intersect_blocks, local_inverse, coarse_basis, coarse_slots, coarse_inverse):
    own, rhs = residuals.shape
    loc, nev = coarse_basis.shape
    rows, width = coarse_inverse.shape
    total = coarse_slots.shape[0]
    nz = ncol // NX
    nplane = nrow * NX
    assert 2 * nev == LANES and rows == ncol * nev and width == nrow * nev and loc == own + 4 * BLK and own % BLK == 0
    packed = (rhs // 2, LANES)
    vmem = pl.BlockSpec(memory_space=pltpu.VMEM)
    hbm = pl.BlockSpec(memory_space=pl.ANY)
    dma = pltpu.SemaphoreType.DMA
    out = pl.pallas_call(
        functools.partial(kernel, nrow, ncol),
        name="schwarz",
        out_shape=pltpu.VMEM((rhs, own), F32),
        in_specs=[hbm] * 6,
        out_specs=vmem,
        scratch_shapes=[
            pltpu.VMEM((rhs, own), BF16),
            pltpu.SMEM(intersect_blocks.shape, jnp.int32),
            pltpu.VMEM((1, total), jnp.int32),
            pltpu.VMEM((4, rhs, BLK), BF16),
            pltpu.VMEM((4, rhs, BLK), BF16),
            pltpu.VMEM((own, loc), BF16),
            pltpu.VMEM((nev, loc), F32),
            pltpu.VMEM((2 * nev, loc), BF16),
            pltpu.VMEM((rows, width), F32),
            pltpu.VMEM((2 * width, rows), BF16),
            pltpu.VMEM((nz * nev, nplane * nev), BF16),
            pltpu.VMEM((nplane * nev, nz * nev), BF16),
            pltpu.VMEM((nplane,) + packed, F32),
            pltpu.VMEM((nz,) + packed, F32),
            pltpu.VMEM((nz,) + packed, F32),
            pltpu.VMEM((nrow,) + packed, F32),
            pltpu.VMEM((ncol,) + packed, F32),
            pltpu.VMEM((ncol,) + packed, F32),
            pltpu.VMEM((nplane,) + packed, F32),
            pltpu.VMEM((nz,) + packed, F32),
            pltpu.VMEM((nz,) + packed, F32),
            pltpu.VMEM((6,) + packed, F32),
            pltpu.VMEM((4, nev, BLK), F32),
            pltpu.VMEM((6 * nev, own), BF16),
            pltpu.VMEM((6 * nev, own), BF16),
            dma((6,)),
            dma((4,)),
            dma((4,)),
            dma((4,)),
            dma((4,)),
            dma((4,)),
            dma((4,)),
            dma((6,)),
            dma((6,)),
        ],
        compiler_params=pltpu.CompilerParams(collective_id=0, has_side_effects=True),
    )(
        residuals.T,
        intersect_blocks,
        local_inverse,
        coarse_basis.T,
        coarse_slots.reshape(1, total),
        coarse_inverse,
    )
    return out.T


def solution(mesh):
    placed = (
        P(("row", "col"), None),
        P(("row", "col"), None),
        P(("row", "col"), None),
        P(("row", "col"), None),
        P(),
        P("row", "col"),
    )
    return jax.shard_map(
        functools.partial(shards, mesh.shape["row"], mesh.shape["col"]),
        mesh=mesh, in_specs=placed, out_specs=P(("row", "col"), None), check_vma=False,
    )
```

```python
import functools

import jax
import jax.numpy as jnp
from jax import lax
from jax.experimental import pallas as pl
from jax.experimental.pallas import tpu as pltpu
from jax.sharding import PartitionSpec as P

MESH = pl.DeviceIdType.MESH
BLK = 128
LANES = 128
NX = 4
CORES = 2
PEAK = 32760.0
STEPS = 8.0
TINY = 1e-30
NT = (((1,), (1,)), ((), ()))
NN = (((1,), (0,)), ((), ()))
F32 = jnp.float32
BF16 = jnp.bfloat16


def matmul(a, b, dims):
    return lax.dot_general(a, b, dims, preferred_element_type=F32)


def split(x):
    hi = x.astype(BF16)
    return hi, (x - hi.astype(F32)).astype(BF16)


def lane_low(shape):
    return lax.broadcasted_iota(jnp.int32, shape, len(shape) - 1) < LANES // 2


def half_roll(x):
    return pltpu.roll(x, LANES // 2, 1)


def far_first(count):
    return sorted(range(1, count), key=lambda k: -min(k, count - k))


def tree_sum(parts):
    while len(parts) > 1:
        parts = [parts[i] + parts[i + 1] if i + 1 < len(parts) else parts[i] for i in range(0, len(parts), 2)]
    return parts[0]


def widest(parts):
    parts = [jnp.abs(p[i:i + 8, q:q + LANES]) for p in parts for i in range(0, p.shape[0], 8) for q in range(0, p.shape[1], LANES)]
    while len(parts) > 1:
        parts = [jnp.maximum(*parts[i:i + 2]) if i + 1 < len(parts) else parts[i] for i in range(0, len(parts), 2)]
    return jnp.max(parts[0], axis=(0, 1), keepdims=True)


def scale_of(parts):
    e = jnp.ceil(jnp.log2(jnp.maximum(widest(parts), TINY)) * STEPS)
    return jnp.broadcast_to(e.astype(jnp.int32), (1, LANES)), jnp.exp2(e * (-1.0 / STEPS)) * PEAK


def scale_from(row):
    return jnp.exp2(row.astype(F32) * (1.0 / STEPS)) * (1.0 / PEAK)


def to_words(top, bot, factor):
    a = jnp.round(top * factor).astype(jnp.int32)
    b = jnp.round(bot * factor).astype(jnp.int32)
    return (a << 16) | (b & 0xFFFF)


def from_words(w):
    return (w >> 16).astype(F32), ((w << 16) >> 16).astype(F32)


def kernel(
    nrow,
    ncol,
    res_hbm,
    ib_hbm,
    linv_hbm,
    basis_hbm,
    slots_hbm,
    coarse_hbm,
    out_ref,
    res_ref,
    ib_ref,
    slots_ref,
    outgoing,
    incoming,
    linv,
    basis,
    basis2,
    coarse,
    coarse_t,
    hot_in,
    hot_out,
    col1,
    row1,
    pieces,
    received,
    col2,
    sets,
    row2,
    lent,
    wide_hi,
    wide_lo,
    load_sem,
    halo_send,
    halo_recv,
    lend_send,
    lend_recv,
    bulk_send,
    bulk_recv,
):
    r = lax.axis_index("row")
    c = lax.axis_index("col")
    z, x = c // NX, lax.rem(c, NX)
    y, core = r // CORES, lax.rem(r, CORES)
    nz, ny = ncol // NX, nrow // CORES
    rhs = res_ref.shape[0]
    own = res_ref.shape[1]
    half = rhs // 2
    quarter = rhs // 4
    rows, width = coarse.shape
    nev = basis.shape[0]
    low = lane_low((quarter, LANES))
    low1 = lane_low((1, LANES))

    col_offsets = sorted(
        ((dz, dx) for dz in range(nz) for dx in range(NX) if (dz, dx) != (0, 0)),
        key=lambda o: -(min(o[0], nz - o[0]) + min(o[1], NX - o[1])))
    row_offsets = sorted(
        ((dy, dk) for dy in range(ny) for dk in range(CORES) if (dy, dk) != (0, 0)),
        key=lambda o: -(min(o[0], ny - o[0]) + 0.5 * o[1]))

    def col_at(dz, dx):
        return lax.rem(z + dz, nz) * NX + lax.rem(x + dx, NX)

    def row_at(dy, dk):
        return lax.rem(y + dy, ny) * CORES + lax.rem(core + dk, CORES)

    exists = [r < nrow - 1, r > 0, c < ncol - 1, c > 0]
    target = [(r + 1, c), (r - 1, c), (r, c + 1), (r, c - 1)]
    opposite = [1, 0, 3, 2]

    barrier = pltpu.get_barrier_semaphore()
    for offset in col_offsets:
        pl.semaphore_signal(barrier, inc=1, device_id=(r, col_at(*offset)), device_id_type=MESH)
    for offset in row_offsets:
        pl.semaphore_signal(barrier, inc=1, device_id=(row_at(*offset), c), device_id_type=MESH)

    loads = [
        pltpu.make_async_copy(basis_hbm, basis, load_sem.at[0]),
        pltpu.make_async_copy(coarse_hbm, coarse, load_sem.at[1]),
        pltpu.make_async_copy(linv_hbm, linv, load_sem.at[2]),
        pltpu.make_async_copy(res_hbm, res_ref, load_sem.at[3]),
        pltpu.make_async_copy(ib_hbm, ib_ref, load_sem.at[4]),
        pltpu.make_async_copy(slots_hbm, slots_ref, load_sem.at[5]),
    ]
    for i in (3, 4, 0, 5, 1, 2):
        loads[i].start()
    loads[4].wait()
    loads[3].wait()

    blocks = [res_ref[:, b * BLK:(b + 1) * BLK] for b in range(own // BLK)]
    for d in range(4):
        index = ib_ref[0, d]
        value = blocks[0]
        for b in range(1, len(blocks)):
            value = jnp.where(index == b, blocks[b], value)
        outgoing[d] = value

        @pl.when(jnp.logical_not(exists[opposite[d]]))
        def _():
            incoming[d] = jnp.zeros_like(incoming[d])

        @pl.when(jnp.logical_not(exists[d]))
        def _():
            lent[d] = jnp.zeros_like(lent[d])

    def halo(d):
        return pltpu.make_async_remote_copy(
            src_ref=outgoing.at[d], dst_ref=incoming.at[d],
            send_sem=halo_send.at[d], recv_sem=halo_recv.at[d],
            device_id=target[d], device_id_type=MESH)

    def lend(d):
        return pltpu.make_async_remote_copy(
            src_ref=basis.at[:, pl.ds(own + d * BLK, BLK)], dst_ref=lent.at[d],
            send_sem=lend_send.at[d], recv_sem=lend_recv.at[d],
            device_id=target[opposite[d]], device_id_type=MESH)

    def send(phase, src, dst, device):
        pltpu.make_async_remote_copy(
            src_ref=src, dst_ref=dst, send_sem=bulk_send.at[phase], recv_sem=bulk_recv.at[phase],
            device_id=device, device_id_type=MESH).start()

    def arrived(phase, buf, count):
        some = buf.at[pl.ds(0, count)]
        pltpu.make_async_copy(some, some, bulk_recv.at[phase]).wait()

    def drained(phase, buf, count):
        some = buf.at[pl.ds(0, count)]
        pltpu.make_async_copy(some, some, bulk_send.at[phase]).wait()

    def spread_col(phase, buf, top, bot):
        row, factor = scale_of([top, bot])
        buf[c, :quarter] = to_words(top, bot, factor)
        buf[c, quarter:] = row
        for offset in col_offsets:
            send(phase, buf.at[c], buf.at[c], (r, col_at(*offset)))

    def gathered(buf):
        columns = []
        for p in range(ncol // 2):
            a, b = buf[2 * p, :quarter], buf[2 * p + 1, :quarter]
            scale = scale_from(jnp.where(low1, buf[2 * p, quarter:], buf[2 * p + 1, quarter:]))
            quarters = from_words(jnp.where(low, a, half_roll(b))) + from_words(jnp.where(low, half_roll(a), b))
            columns.append(jnp.concatenate([q * scale for q in quarters], axis=0))
        return jnp.concatenate(split(jnp.concatenate(columns, axis=1)), axis=0)

    def paired_words(part, factor):
        first = to_words(part[:quarter], part[quarter:half], factor)
        second = to_words(part[half:half + quarter], part[half + quarter:], factor)
        return jnp.where(low, first, half_roll(second)), jnp.where(low, half_roll(first), second)

    pl.semaphore_wait(barrier, ncol + nrow - 2)
    for d in range(4):
        @pl.when(exists[d])
        def _():
            halo(d).start()

    loads[5].wait()
    chunk = 2 * LANES
    place_in = lax.broadcasted_iota(jnp.int32, (width, chunk), 0) + c * width

    def build_in(i, carry):
        slot = slots_ref[:, pl.ds(pl.multiple_of(r * rows + i * chunk, chunk), chunk)]
        hot = jnp.where(place_in == slot, 1.0, 0.0).astype(BF16)
        hot_in[pl.ds(pl.multiple_of(i * chunk, chunk), chunk)] = hot.T
        return carry

    lax.fori_loop(0, rows // chunk, build_in, 0)
    loads[0].wait()
    b_hi, b_lo = split(basis[...])
    basis2[:nev] = b_hi
    basis2[nev:] = b_lo
    partial = matmul(res_ref[...], basis2[:, :own], NT)

    for d in range(4):
        @pl.when(exists[opposite[d]])
        def _():
            halo(d).wait_recv()

    inc = jnp.concatenate([incoming[d] for d in range(4)], axis=1)
    partial = partial + matmul(inc, basis2[:, own:], NT)
    partial = partial + half_roll(partial)
    spread_col(0, col1, jnp.where(low, partial[:quarter], partial[half:half + quarter]),
               jnp.where(low, partial[quarter:half], partial[half + quarter:]))

    span = rows // nz
    loads[1].wait()
    for t in range(nz):
        at = slice(t * span, (t + 1) * span)
        coarse_t[:width, at], coarse_t[width:, at] = split(coarse[at].T)
    loads[2].wait()
    local = jnp.concatenate([res_ref[...], inc], axis=1)
    out_ref[...] = matmul(local, linv[...], NT)

    arrived(0, col1, ncol - 1)
    part = matmul(gathered(col1), hot_in[...], NN)
    part = part[:rhs] + part[rhs:]
    row, factor = scale_of([part])
    blocks4 = width // LANES
    for q in range(blocks4):
        at = slice(q * LANES, (q + 1) * LANES)
        row1[r, q * half:(q + 1) * half] = to_words(part[:half, at], part[half:, at], factor)
    row1[r, blocks4 * half:] = row
    for offset in row_offsets:
        send(1, row1.at[r], row1.at[r], (row_at(*offset), c))

    low8 = lane_low((8, LANES))
    wanted = []
    for column, valid in ((c, None), (c + 1, exists[2]), (c - 1, exists[3])):
        safe = jnp.clip(column, 0, ncol - 1)
        for t in range(nrow // 2):
            pair = []
            for device in (2 * t * ncol + safe, (2 * t + 1) * ncol + safe):
                at = pl.ds(pl.multiple_of((device // 2) * LANES, LANES), LANES)
                pair.append(jnp.broadcast_to(slots_ref[:, at], (8, LANES)))
            even = jnp.where(low8, pair[0], half_roll(pair[1]))
            odd = jnp.where(low8, half_roll(pair[0]), pair[1])
            both = jnp.where(lax.rem(safe, 2) == 0, even, odd)[:1]
            wanted.append(both if valid is None else jnp.where(valid, both, -1))
    wanted = jnp.concatenate(wanted, axis=1) - r * rows
    place_out = lax.broadcasted_iota(jnp.int32, (LANES, wanted.shape[1]), 0)

    def build_out(i, carry):
        hot = jnp.where(place_out == wanted - i * LANES, 1.0, 0.0)
        hot_out[pl.ds(pl.multiple_of(i * LANES, LANES), LANES)] = hot.astype(BF16)
        return carry

    lax.fori_loop(0, rows // LANES, build_out, 0)

    arrived(1, row1, nrow - 1)
    scales = [scale_from(row1[i, blocks4 * half:]) for i in range(nrow)]
    column = []
    for q in range(blocks4):
        tops, bots = [], []
        for i in range(nrow):
            top, bot = from_words(row1[i, q * half:(q + 1) * half])
            tops.append(top * scales[i])
            bots.append(bot * scales[i])
        column.append(jnp.concatenate([tree_sum(tops), tree_sum(bots)], axis=0))
    column2 = jnp.concatenate(split(jnp.concatenate(column, axis=1)), axis=0)
    column4 = jnp.concatenate([column2, column2], axis=1)

    steps = far_first(nz) + [0]
    for batch in (steps[:nz // 2], steps[nz // 2:]):
        parts = []
        for dz in batch:
            block = lax.rem(z + dz, nz)
            at = pl.ds(pl.multiple_of(block * span, span), span)
            part = matmul(column4, coarse_t[:, at], NN)
            parts.append((block, part[:rhs] + part[rhs:]))
        row, factor = scale_of([part for block, part in parts])
        for block, part in parts:
            for q in range(span // LANES):
                pair = paired_words(part[:, q * LANES:(q + 1) * LANES], factor)
                for i in range(2):
                    pieces[block * NX + 2 * q + i, :quarter] = pair[i]
                    pieces[block * NX + 2 * q + i, quarter:] = row
        for dz, (block, part) in zip(batch, parts):
            for dx in (2, 1, 3, 0) if dz else (2, 1, 3):
                to = block * NX + lax.rem(x + dx, NX)
                send(2, pieces.at[to], received.at[c], (r, to))

    for d in range(4):
        @pl.when(exists[opposite[d]])
        def _():
            lend(d).start()

    received[c] = pieces[c]
    arrived(2, received, ncol - 1)
    tops, bots = [], []
    for i in range(ncol):
        scale = scale_from(received[i, quarter:])
        top, bot = from_words(received[i, :quarter])
        tops.append(top * scale)
        bots.append(bot * scale)
    top, bot = tree_sum(tops), tree_sum(bots)
    spread_col(3, col2, top, bot)

    wide_hi[:nev] = basis2[:nev, :own]
    wide_lo[:nev] = basis2[nev:, :own]
    wide_hi[5 * nev:] = jnp.zeros_like(wide_hi[5 * nev:])
    wide_lo[5 * nev:] = jnp.zeros_like(wide_lo[5 * nev:])
    for d in range(4):
        @pl.when(exists[d])
        def _():
            lend(d).wait_recv()

        l_hi, l_lo = split(lent[d])
        for b in range(own // BLK):
            here = ib_ref[0, d] == b
            at = slice((d + 1) * nev, (d + 2) * nev), slice(b * BLK, (b + 1) * BLK)
            wide_hi[at] = jnp.where(here, l_hi, jnp.zeros_like(l_hi))
            wide_lo[at] = jnp.where(here, l_lo, jnp.zeros_like(l_lo))

    arrived(3, col2, ncol - 1)
    part = matmul(gathered(col2), hot_out[...], NN)
    part = part[:rhs] + part[rhs:]
    row, factor = scale_of([part])
    words = []
    for q in range(part.shape[1] // LANES):
        words.extend(paired_words(part[:, q * LANES:(q + 1) * LANES], factor))
    for i in range(nrow):
        near = (i, min(i + 1, nrow - 1), max(i - 1, 0), nrow + i, 2 * nrow + i)
        for k, index in enumerate(near):
            sets[i, k * quarter:(k + 1) * quarter] = words[index]
        sets[i, 5 * quarter:] = row
    for offset in row_offsets:
        to = row_at(*offset)
        send(4, sets.at[to], row2.at[r], (to, c))
    row2[r] = sets[r]
    arrived(4, row2, nrow - 1)
    scales = [scale_from(row2[i, 5 * quarter:]) for i in range(nrow)]
    picks = []
    for k in range(5):
        tops, bots = [], []
        for i in range(nrow):
            top, bot = from_words(row2[i, k * quarter:(k + 1) * quarter])
            tops.append(top * scales[i])
            bots.append(bot * scales[i])
        picks.append((tree_sum(tops), tree_sum(bots)))
    picks.append((jnp.zeros_like(picks[0][0]),) * 2)
    columns = []
    for p in range(3):
        a, b = picks[2 * p], picks[2 * p + 1]
        columns.append(jnp.concatenate(
            [jnp.where(low, a[i], half_roll(b[i])) for i in range(2)]
            + [jnp.where(low, half_roll(a[i]), b[i]) for i in range(2)], axis=0))
    picked = jnp.concatenate(split(jnp.concatenate(columns, axis=1)), axis=0)
    inner = matmul(picked, wide_hi[...], NN) + matmul(picked, wide_lo[...], NN)
    out_ref[...] = out_ref[...] + inner[:rhs] + inner[rhs:]

    drained(0, col1, ncol - 1)
    drained(1, row1, nrow - 1)
    drained(2, received, ncol - 1)
    drained(3, col2, ncol - 1)
    drained(4, row2, nrow - 1)
    for d in range(4):
        @pl.when(exists[d])
        def _():
            halo(d).wait_send()

        @pl.when(exists[opposite[d]])
        def _():
            lend(d).wait_send()


def shards(nrow, ncol, residuals, intersect_blocks, local_inverse, coarse_basis, coarse_slots, coarse_inverse):
    own, rhs = residuals.shape
    loc, nev = coarse_basis.shape
    rows, width = coarse_inverse.shape
    total = coarse_slots.shape[0]
    assert 2 * nev == LANES and rows == ncol * nev and width == nrow * nev and loc == own + 4 * BLK and own % BLK == 0
    vmem = pl.BlockSpec(memory_space=pltpu.VMEM)
    hbm = pl.BlockSpec(memory_space=pl.ANY)
    dma = pltpu.SemaphoreType.DMA
    out = pl.pallas_call(
        functools.partial(kernel, nrow, ncol),
        name="schwarz",
        out_shape=pltpu.VMEM((rhs, own), F32),
        in_specs=[hbm] * 6,
        out_specs=vmem,
        scratch_shapes=[
            pltpu.VMEM((rhs, own), BF16),
            pltpu.SMEM(intersect_blocks.shape, jnp.int32),
            pltpu.VMEM((1, total), jnp.int32),
            pltpu.VMEM((4, rhs, BLK), BF16),
            pltpu.VMEM((4, rhs, BLK), BF16),
            pltpu.VMEM((own, loc), BF16),
            pltpu.VMEM((nev, loc), F32),
            pltpu.VMEM((2 * nev, loc), BF16),
            pltpu.VMEM((rows, width), F32),
            pltpu.VMEM((2 * width, rows), BF16),
            pltpu.VMEM((rows, width), BF16),
            pltpu.VMEM((rows, 3 * width), BF16),
            pltpu.VMEM((ncol, rhs // 4 + 1, LANES), jnp.int32),
            pltpu.VMEM((nrow, width // LANES * (rhs // 2) + 1, LANES), jnp.int32),
            pltpu.VMEM((ncol, rhs // 4 + 1, LANES), jnp.int32),
            pltpu.VMEM((ncol, rhs // 4 + 1, LANES), jnp.int32),
            pltpu.VMEM((ncol, rhs // 4 + 1, LANES), jnp.int32),
            pltpu.VMEM((nrow, 5 * (rhs // 4) + 1, LANES), jnp.int32),
            pltpu.VMEM((nrow, 5 * (rhs // 4) + 1, LANES), jnp.int32),
            pltpu.VMEM((4, nev, BLK), F32),
            pltpu.VMEM((6 * nev, own), BF16),
            pltpu.VMEM((6 * nev, own), BF16),
            dma((6,)),
            dma((4,)),
            dma((4,)),
            dma((4,)),
            dma((4,)),
            dma((5,)),
            dma((5,)),
        ],
        compiler_params=pltpu.CompilerParams(collective_id=0, has_side_effects=True),
    )(
        residuals.T,
        intersect_blocks,
        local_inverse,
        coarse_basis.T,
        coarse_slots.reshape(1, total),
        coarse_inverse,
    )
    return out.T


def solution(mesh):
    placed = (
        P(("row", "col"), None),
        P(("row", "col"), None),
        P(("row", "col"), None),
        P(("row", "col"), None),
        P(),
        P("row", "col"),
    )
    return jax.shard_map(
        functools.partial(shards, mesh.shape["row"], mesh.shape["col"]),
        mesh=mesh, in_specs=placed, out_specs=P(("row", "col"), None), check_vma=False,
    )
```

```python
import functools

import jax
import jax.numpy as jnp
from jax import lax
from jax.experimental import pallas as pl
from jax.experimental.pallas import tpu as pltpu
from jax.sharding import PartitionSpec as P

MESH = pl.DeviceIdType.MESH
BLK = 128
LANES = 128
NX = 4
CORES = 2
PEAK = 32760.0
STEPS = 8.0
TINY = 1e-30
NT = (((1,), (1,)), ((), ()))
NN = (((1,), (0,)), ((), ()))
F32 = jnp.float32
BF16 = jnp.bfloat16


def matmul(a, b, dims):
    return lax.dot_general(a, b, dims, preferred_element_type=F32)


def split(x):
    hi = x.astype(BF16)
    return hi, (x - hi.astype(F32)).astype(BF16)


def lane_low(shape):
    return lax.broadcasted_iota(jnp.int32, shape, len(shape) - 1) < LANES // 2


def half_roll(x):
    return pltpu.roll(x, LANES // 2, 1)


def far_first(count):
    return sorted(range(1, count), key=lambda k: -min(k, count - k))


def tree_sum(parts):
    while len(parts) > 1:
        parts = [parts[i] + parts[i + 1] if i + 1 < len(parts) else parts[i] for i in range(0, len(parts), 2)]
    return parts[0]


def scale_of(largest):
    top = jnp.broadcast_to(jnp.max(largest, axis=0, keepdims=True), largest.shape)
    e = jnp.ceil(jnp.log2(jnp.maximum(top, TINY)) * STEPS)
    return e.astype(jnp.int32), jnp.exp2(e * (-1.0 / STEPS)) * PEAK


def scale_from(row):
    return jnp.exp2(row.astype(F32) * (1.0 / STEPS)) * (1.0 / PEAK)


def to_words(top, bot, factor):
    a = jnp.round(top * factor).astype(jnp.int32)
    b = jnp.round(bot * factor).astype(jnp.int32)
    return (a << 16) | (b & 0xFFFF)


def from_words(w):
    return (w >> 16).astype(F32), ((w << 16) >> 16).astype(F32)


def kernel(
    nrow,
    ncol,
    res_hbm,
    ib_hbm,
    linv_hbm,
    basis_hbm,
    slots_hbm,
    coarse_hbm,
    out_ref,
    res_ref,
    ib_ref,
    slots_ref,
    outgoing,
    incoming,
    linv,
    basis,
    basis2,
    coarse,
    coarse_t,
    hot_in,
    hot_out,
    col1,
    row1,
    pieces,
    received,
    col2,
    sets,
    row2,
    lent,
    wide_hi,
    wide_lo,
    load_sem,
    halo_send,
    halo_recv,
    lend_send,
    lend_recv,
    bulk_send,
    bulk_recv,
    passed,
):
    r = lax.axis_index("row")
    c = lax.axis_index("col")
    z, x = c // NX, lax.rem(c, NX)
    y, core = r // CORES, lax.rem(r, CORES)
    nz, ny = ncol // NX, nrow // CORES
    rhs = res_ref.shape[0]
    own = res_ref.shape[1]
    half = rhs // 2
    quarter = rhs // 4
    rows, width = coarse.shape
    nev = basis.shape[0]
    low = lane_low((quarter, LANES))
    low1 = lane_low((1, LANES))

    col_offsets = sorted(
        ((dz, dx) for dz in range(nz) for dx in range(NX) if (dz, dx) != (0, 0)),
        key=lambda o: -(min(o[0], nz - o[0]) + min(o[1], NX - o[1])))
    row_offsets = sorted(
        ((dy, dk) for dy in range(ny) for dk in range(CORES) if (dy, dk) != (0, 0)),
        key=lambda o: -(min(o[0], ny - o[0]) + 0.5 * o[1]))

    def col_at(dz, dx):
        return lax.rem(z + dz, nz) * NX + lax.rem(x + dx, NX)

    def row_at(dy, dk):
        return lax.rem(y + dy, ny) * CORES + lax.rem(core + dk, CORES)

    exists = [r < nrow - 1, r > 0, c < ncol - 1, c > 0]
    target = [(r + 1, c), (r - 1, c), (r, c + 1), (r, c - 1)]
    opposite = [1, 0, 3, 2]

    loads = [
        pltpu.make_async_copy(basis_hbm, basis, load_sem.at[0]),
        pltpu.make_async_copy(coarse_hbm, coarse, load_sem.at[1]),
        pltpu.make_async_copy(linv_hbm, linv, load_sem.at[2]),
        pltpu.make_async_copy(res_hbm, res_ref, load_sem.at[3]),
        pltpu.make_async_copy(ib_hbm, ib_ref, load_sem.at[4]),
        pltpu.make_async_copy(slots_hbm, slots_ref, load_sem.at[5]),
    ]
    for i in (3, 4, 0):
        loads[i].start()

    def line_x(dx):
        return (r, z * NX + lax.rem(x + dx, NX))

    def line_z(dz):
        return (r, lax.rem(z + dz, nz) * NX + x)

    across_x = [line_x(dx) for dx in (1, NX - 1, 2)]
    near_z = [line_z(dz) for dz in (1, nz - 1, 2, nz - 2)]
    up = jnp.logical_and(x == NX - 1, exists[2])
    down = jnp.logical_and(x == 0, exists[3])
    barrier = pltpu.get_barrier_semaphore()

    def signal(sem, device):
        pl.semaphore_signal(sem, inc=1, device_id=device, device_id_type=MESH)

    @pl.when(up)
    def _():
        signal(barrier, target[2])

    @pl.when(down)
    def _():
        signal(barrier, target[3])

    for offset in row_offsets:
        signal(barrier, (row_at(*offset), c))
    for device in across_x + near_z:
        signal(barrier, device)
    for i in (5, 1, 2):
        loads[i].start()
    loads[4].wait()
    loads[3].wait()

    blocks = [res_ref[:, b * BLK:(b + 1) * BLK] for b in range(own // BLK)]
    for d in range(4):
        index = ib_ref[0, d]
        value = blocks[0]
        for b in range(1, len(blocks)):
            value = jnp.where(index == b, blocks[b], value)
        outgoing[d] = value

        @pl.when(jnp.logical_not(exists[opposite[d]]))
        def _():
            incoming[d] = jnp.zeros_like(incoming[d])

        @pl.when(jnp.logical_not(exists[d]))
        def _():
            lent[d] = jnp.zeros_like(lent[d])

    def halo(d):
        return pltpu.make_async_remote_copy(
            src_ref=outgoing.at[d], dst_ref=incoming.at[d],
            send_sem=halo_send.at[d], recv_sem=halo_recv.at[d],
            device_id=target[d], device_id_type=MESH)

    def lend(d):
        return pltpu.make_async_remote_copy(
            src_ref=basis.at[:, pl.ds(own + d * BLK, BLK)], dst_ref=lent.at[d],
            send_sem=lend_send.at[d], recv_sem=lend_recv.at[d],
            device_id=target[opposite[d]], device_id_type=MESH)

    def send(phase, src, dst, device):
        pltpu.make_async_remote_copy(
            src_ref=src, dst_ref=dst, send_sem=bulk_send.at[phase], recv_sem=bulk_recv.at[phase],
            device_id=device, device_id_type=MESH).start()

    def arrived(phase, buf, count):
        some = buf.at[pl.ds(0, count)]
        pltpu.make_async_copy(some, some, bulk_recv.at[phase]).wait()

    def drained(phase, buf, count):
        some = buf.at[pl.ds(0, count)]
        pltpu.make_async_copy(some, some, bulk_send.at[phase]).wait()

    plane = NX * nev
    near = 5

    def plane_at(k):
        return lax.rem(z + (k + 1) // 2 * (2 * (k % 2) - 1) + nz, nz)

    def is_far(dz):
        return min(dz, nz - dz) > near // 2

    def spread_col(phase, buf, top, bot, ready):
        largest = jnp.maximum(jnp.abs(top), jnp.abs(bot))
        e, factor = scale_of(jnp.maximum(largest, half_roll(largest)))
        buf[c, :quarter] = to_words(top, bot, factor)
        buf[c, quarter:] = e[:1]
        ready()
        for dz, dx in col_offsets:
            send(phase + is_far(dz), buf.at[c], buf.at[c], (r, col_at(dz, dx)))

    def gathered(buf, planes):
        columns = []
        for k in planes:
            for q in range(0, NX, 2):
                first = plane_at(k) * NX + q
                a, b = buf[first, :quarter], buf[first + 1, :quarter]
                scale = scale_from(jnp.where(low1, buf[first, quarter:], buf[first + 1, quarter:]))
                quarters = from_words(jnp.where(low, a, half_roll(b))) + from_words(jnp.where(low, half_roll(a), b))
                columns.append(jnp.concatenate([v * scale for v in quarters], axis=0))
        return jnp.concatenate(split(jnp.concatenate(columns, axis=1)), axis=0)

    def select(phase, buf, hot):
        arrived(phase, buf, near * NX - 1)
        part = matmul(gathered(buf, range(near)), hot[:near * plane], NN)
        arrived(phase + 1, buf, (nz - near) * NX)
        part = part + matmul(gathered(buf, range(near, nz)), hot[near * plane:], NN)
        return part[:rhs] + part[rhs:]

    def largest_of(part):
        return functools.reduce(jnp.maximum, [jnp.abs(part[i:i + quarter]) for i in range(0, rhs, quarter)])

    def paired_words(part):
        e, factor = scale_of(largest_of(part))
        first = to_words(part[:quarter], part[quarter:half], factor)
        second = to_words(part[half:half + quarter], part[half + quarter:], factor)
        swapped = half_roll(e)
        return ((jnp.where(low, first, half_roll(second)), jnp.where(low, e, swapped)[:1]),
                (jnp.where(low, half_roll(first), second), jnp.where(low, swapped, e)[:1]))

    pl.semaphore_wait(barrier, nrow - 1 + len(across_x) + len(near_z) + up.astype(jnp.int32) + down.astype(jnp.int32))
    for d in range(4):
        @pl.when(exists[d])
        def _():
            halo(d).start()

    for device in across_x + near_z:
        signal(passed.at[0], device)
    loads[0].wait()
    b_hi, b_lo = split(basis[...])
    basis2[:nev] = b_hi
    basis2[nev:] = b_lo
    partial = matmul(res_ref[...], basis2[:, :own], NT)
    pl.semaphore_wait(passed.at[0], len(across_x) + len(near_z))
    for device in across_x:
        signal(passed.at[1], device)

    for d in range(4):
        @pl.when(exists[opposite[d]])
        def _():
            halo(d).wait_recv()

    inc = jnp.concatenate([incoming[d] for d in range(4)], axis=1)
    partial = partial + matmul(inc, basis2[:, own:], NT)
    partial = partial + half_roll(partial)
    spread_col(0, col1, jnp.where(low, partial[:quarter], partial[half:half + quarter]),
               jnp.where(low, partial[quarter:half], partial[half + quarter:]),
               lambda: pl.semaphore_wait(passed.at[1], len(across_x)))

    span = rows // nz
    loads[1].wait()
    for t in range(nz):
        at = slice(t * span, (t + 1) * span)
        coarse_t[:width, at], coarse_t[width:, at] = split(coarse[at].T)
    loads[2].wait()
    local = jnp.concatenate([res_ref[...], inc], axis=1)
    out_ref[...] = matmul(local, linv[...], NT)

    loads[5].wait()
    place_in = lax.broadcasted_iota(jnp.int32, (width, plane), 0) + c * width

    def build_in(k, carry):
        slot = slots_ref[:, pl.ds(pl.multiple_of(r * rows + plane_at(k) * plane, plane), plane)]
        hot = jnp.where(place_in == slot, 1.0, 0.0).astype(BF16)
        hot_in[pl.ds(pl.multiple_of(k * plane, plane), plane)] = hot.T
        return carry

    lax.fori_loop(0, nz, build_in, 0)

    part = select(0, col1, hot_in)
    blocks4 = width // LANES
    for q in range(blocks4):
        block = part[:, q * LANES:(q + 1) * LANES]
        e, factor = scale_of(largest_of(block))
        row1[r, q * half:(q + 1) * half] = to_words(block[:half], block[half:], factor[:1])
        row1[r, blocks4 * half + q:blocks4 * half + q + 1] = e[:1]
    for offset in row_offsets:
        send(2, row1.at[r], row1.at[r], (row_at(*offset), c))

    low8 = lane_low((8, LANES))
    wanted = []
    for column, valid in ((c, None), (c + 1, exists[2]), (c - 1, exists[3])):
        safe = jnp.clip(column, 0, ncol - 1)
        for t in range(nrow // 2):
            pair = []
            for device in (2 * t * ncol + safe, (2 * t + 1) * ncol + safe):
                at = pl.ds(pl.multiple_of((device // 2) * LANES, LANES), LANES)
                pair.append(jnp.broadcast_to(slots_ref[:, at], (8, LANES)))
            even = jnp.where(low8, pair[0], half_roll(pair[1]))
            odd = jnp.where(low8, half_roll(pair[0]), pair[1])
            both = jnp.where(lax.rem(safe, 2) == 0, even, odd)[:1]
            wanted.append(both if valid is None else jnp.where(valid, both, -1))
    wanted = jnp.concatenate(wanted, axis=1) - r * rows
    place_out = lax.broadcasted_iota(jnp.int32, (LANES, wanted.shape[1]), 0)

    def build_out(i, carry):
        start = plane_at(i // 2) * plane + i % 2 * LANES
        hot = jnp.where(place_out == wanted - start, 1.0, 0.0)
        hot_out[pl.ds(pl.multiple_of(i * LANES, LANES), LANES)] = hot.astype(BF16)
        return carry

    lax.fori_loop(0, rows // LANES, build_out, 0)

    arrived(2, row1, nrow - 1)
    column = []
    for q in range(blocks4):
        tops, bots = [], []
        for i in range(nrow):
            scale = scale_from(row1[i, blocks4 * half + q:blocks4 * half + q + 1])
            top, bot = from_words(row1[i, q * half:(q + 1) * half])
            tops.append(top * scale)
            bots.append(bot * scale)
        column.append(jnp.concatenate([tree_sum(tops), tree_sum(bots)], axis=0))
    column2 = jnp.concatenate(split(jnp.concatenate(column, axis=1)), axis=0)
    column4 = jnp.concatenate([column2, column2], axis=1)

    steps = far_first(nz) + [0]
    for batch in (steps[:2], steps[2:5], steps[5:]):
        parts = []
        for dz in batch:
            block = lax.rem(z + dz, nz)
            at = pl.ds(pl.multiple_of(block * span, span), span)
            part = matmul(column4, coarse_t[:, at], NN)
            parts.append((block, part[:rhs] + part[rhs:]))
        for block, part in parts:
            for q in range(span // LANES):
                for i, (words, e) in enumerate(paired_words(part[:, q * LANES:(q + 1) * LANES])):
                    pieces[block * NX + 2 * q + i, :quarter] = words
                    pieces[block * NX + 2 * q + i, quarter:] = e
        for dz, (block, part) in zip(batch, parts):
            for dx in (2, 1, 3, 0) if dz else (2, 1, 3):
                to = block * NX + lax.rem(x + dx, NX)
                send(3, pieces.at[to], received.at[c], (r, to))

    for d in range(4):
        @pl.when(exists[opposite[d]])
        def _():
            lend(d).start()

    received[c] = pieces[c]
    arrived(3, received, ncol - 1)
    tops, bots = [], []
    for i in range(ncol):
        scale = scale_from(received[i, quarter:])
        top, bot = from_words(received[i, :quarter])
        tops.append(top * scale)
        bots.append(bot * scale)
    top, bot = tree_sum(tops), tree_sum(bots)
    spread_col(4, col2, top, bot, lambda: None)

    wide_hi[:nev] = basis2[:nev, :own]
    wide_lo[:nev] = basis2[nev:, :own]
    wide_hi[5 * nev:] = jnp.zeros_like(wide_hi[5 * nev:])
    wide_lo[5 * nev:] = jnp.zeros_like(wide_lo[5 * nev:])
    for d in range(4):
        @pl.when(exists[d])
        def _():
            lend(d).wait_recv()

        l_hi, l_lo = split(lent[d])
        for b in range(own // BLK):
            here = ib_ref[0, d] == b
            at = slice((d + 1) * nev, (d + 2) * nev), slice(b * BLK, (b + 1) * BLK)
            wide_hi[at] = jnp.where(here, l_hi, jnp.zeros_like(l_hi))
            wide_lo[at] = jnp.where(here, l_lo, jnp.zeros_like(l_lo))

    part = select(4, col2, hot_out)
    groups = []
    for q in range(part.shape[1] // LANES):
        groups.extend(paired_words(part[:, q * LANES:(q + 1) * LANES]))
    for i in range(nrow):
        around = (i, min(i + 1, nrow - 1), max(i - 1, 0), nrow + i, 2 * nrow + i)
        for k, index in enumerate(around):
            sets[i, k * quarter:(k + 1) * quarter], sets[i, 5 * quarter + k:5 * quarter + k + 1] = groups[index]
    for offset in row_offsets:
        to = row_at(*offset)
        send(6, sets.at[to], row2.at[r], (to, c))
    row2[r] = sets[r]
    arrived(6, row2, nrow - 1)
    picks = []
    for k in range(5):
        tops, bots = [], []
        for i in range(nrow):
            scale = scale_from(row2[i, 5 * quarter + k:5 * quarter + k + 1])
            top, bot = from_words(row2[i, k * quarter:(k + 1) * quarter])
            tops.append(top * scale)
            bots.append(bot * scale)
        picks.append((tree_sum(tops), tree_sum(bots)))
    picks.append((jnp.zeros_like(picks[0][0]),) * 2)
    columns = []
    for p in range(3):
        a, b = picks[2 * p], picks[2 * p + 1]
        columns.append(jnp.concatenate(
            [jnp.where(low, a[i], half_roll(b[i])) for i in range(2)]
            + [jnp.where(low, half_roll(a[i]), b[i]) for i in range(2)], axis=0))
    picked = jnp.concatenate(split(jnp.concatenate(columns, axis=1)), axis=0)
    inner = matmul(picked, wide_hi[...], NN) + matmul(picked, wide_lo[...], NN)
    out_ref[...] = out_ref[...] + inner[:rhs] + inner[rhs:]

    for phase, buf in ((0, col1), (4, col2)):
        drained(phase, buf, near * NX - 1)
        drained(phase + 1, buf, (nz - near) * NX)
    drained(2, row1, nrow - 1)
    drained(3, received, ncol - 1)
    drained(6, row2, nrow - 1)
    for d in range(4):
        @pl.when(exists[d])
        def _():
            halo(d).wait_send()

        @pl.when(exists[opposite[d]])
        def _():
            lend(d).wait_send()


def shards(nrow, ncol, residuals, intersect_blocks, local_inverse, coarse_basis, coarse_slots, coarse_inverse):
    own, rhs = residuals.shape
    loc, nev = coarse_basis.shape
    rows, width = coarse_inverse.shape
    total = coarse_slots.shape[0]
    assert 2 * nev == LANES and rows == ncol * nev and width == nrow * nev and loc == own + 4 * BLK and own % BLK == 0
    vmem = pl.BlockSpec(memory_space=pltpu.VMEM)
    hbm = pl.BlockSpec(memory_space=pl.ANY)
    dma = pltpu.SemaphoreType.DMA
    out = pl.pallas_call(
        functools.partial(kernel, nrow, ncol),
        name="schwarz",
        out_shape=pltpu.VMEM((rhs, own), F32),
        in_specs=[hbm] * 6,
        out_specs=vmem,
        scratch_shapes=[
            pltpu.VMEM((rhs, own), BF16),
            pltpu.SMEM(intersect_blocks.shape, jnp.int32),
            pltpu.VMEM((1, total), jnp.int32),
            pltpu.VMEM((4, rhs, BLK), BF16),
            pltpu.VMEM((4, rhs, BLK), BF16),
            pltpu.VMEM((own, loc), BF16),
            pltpu.VMEM((nev, loc), F32),
            pltpu.VMEM((2 * nev, loc), BF16),
            pltpu.VMEM((rows, width), F32),
            pltpu.VMEM((2 * width, rows), BF16),
            pltpu.VMEM((rows, width), BF16),
            pltpu.VMEM((rows, 3 * width), BF16),
            pltpu.VMEM((ncol, rhs // 4 + 1, LANES), jnp.int32),
            pltpu.VMEM((nrow, width // LANES * (rhs // 2 + 1), LANES), jnp.int32),
            pltpu.VMEM((ncol, rhs // 4 + 1, LANES), jnp.int32),
            pltpu.VMEM((ncol, rhs // 4 + 1, LANES), jnp.int32),
            pltpu.VMEM((ncol, rhs // 4 + 1, LANES), jnp.int32),
            pltpu.VMEM((nrow, 5 * (rhs // 4 + 1), LANES), jnp.int32),
            pltpu.VMEM((nrow, 5 * (rhs // 4 + 1), LANES), jnp.int32),
            pltpu.VMEM((4, nev, BLK), F32),
            pltpu.VMEM((6 * nev, own), BF16),
            pltpu.VMEM((6 * nev, own), BF16),
            dma((6,)),
            dma((4,)),
            dma((4,)),
            dma((4,)),
            dma((4,)),
            dma((7,)),
            dma((7,)),
            pltpu.SemaphoreType.REGULAR((2,)),
        ],
        compiler_params=pltpu.CompilerParams(collective_id=0, has_side_effects=True),
    )(
        residuals.T,
        intersect_blocks,
        local_inverse,
        coarse_basis.T,
        coarse_slots.reshape(1, total),
        coarse_inverse,
    )
    return out.T


def solution(mesh):
    placed = (
        P(("row", "col"), None),
        P(("row", "col"), None),
        P(("row", "col"), None),
        P(("row", "col"), None),
        P(),
        P("row", "col"),
    )
    return jax.shard_map(
        functools.partial(shards, mesh.shape["row"], mesh.shape["col"]),
        mesh=mesh, in_specs=placed, out_specs=P(("row", "col"), None), check_vma=False,
    )
```

```python
import functools

import jax
import jax.numpy as jnp
from jax import lax
from jax.experimental import pallas as pl
from jax.experimental.pallas import tpu as pltpu
from jax.sharding import PartitionSpec as P

MESH = pl.DeviceIdType.MESH
BLK = 128
LANES = 128
NX = 4
CORES = 2
PEAK = 32760.0
STEPS = 8.0
TINY = 1e-30
NT = (((1,), (1,)), ((), ()))
NN = (((1,), (0,)), ((), ()))
F32 = jnp.float32
BF16 = jnp.bfloat16


def matmul(a, b, dims):
    return lax.dot_general(a, b, dims, preferred_element_type=F32)


def split(x):
    hi = x.astype(BF16)
    return hi, (x - hi.astype(F32)).astype(BF16)


def lane_low(shape):
    return lax.broadcasted_iota(jnp.int32, shape, len(shape) - 1) < LANES // 2


def half_roll(x):
    return pltpu.roll(x, LANES // 2, 1)


def far_first(count):
    return sorted(range(1, count), key=lambda k: -min(k, count - k))


def tree_sum(parts):
    while len(parts) > 1:
        parts = [parts[i] + parts[i + 1] if i + 1 < len(parts) else parts[i] for i in range(0, len(parts), 2)]
    return parts[0]


def scale_of(largest):
    top = jnp.broadcast_to(jnp.max(largest, axis=0, keepdims=True), largest.shape)
    e = jnp.ceil(jnp.log2(jnp.maximum(top, TINY)) * STEPS)
    return e.astype(jnp.int32), jnp.exp2(e * (-1.0 / STEPS)) * PEAK


def scale_from(row):
    return jnp.exp2(row.astype(F32) * (1.0 / STEPS)) * (1.0 / PEAK)


def to_words(top, bot, factor):
    a = jnp.round(top * factor).astype(jnp.int32)
    b = jnp.round(bot * factor).astype(jnp.int32)
    return (a << 16) | (b & 0xFFFF)


def from_words(w):
    return (w >> 16).astype(F32), ((w << 16) >> 16).astype(F32)


def kernel(
    nrow,
    ncol,
    res_hbm,
    ib_hbm,
    linv_hbm,
    basis_hbm,
    slots_hbm,
    coarse_hbm,
    out_ref,
    res_ref,
    ib_ref,
    slots_ref,
    outgoing,
    incoming,
    linv,
    basis,
    basis2,
    coarse,
    coarse_t,
    hot_in,
    hot_out,
    col1,
    row1,
    pieces,
    received,
    col2,
    sets,
    row2,
    lent,
    wide_hi,
    wide_lo,
    load_sem,
    halo_send,
    halo_recv,
    lend_send,
    lend_recv,
    bulk_send,
    bulk_recv,
    passed,
):
    r = lax.axis_index("row")
    c = lax.axis_index("col")
    z, x = c // NX, lax.rem(c, NX)
    y, core = r // CORES, lax.rem(r, CORES)
    nz, ny = ncol // NX, nrow // CORES
    rhs = res_ref.shape[0]
    own = res_ref.shape[1]
    half = rhs // 2
    quarter = rhs // 4
    rows, width = coarse.shape
    nev = basis.shape[0]
    low = lane_low((quarter, LANES))
    low1 = lane_low((1, LANES))

    col_offsets = sorted(
        ((dz, dx) for dz in range(nz) for dx in range(NX) if (dz, dx) != (0, 0)),
        key=lambda o: -(min(o[0], nz - o[0]) + min(o[1], NX - o[1])))
    row_offsets = sorted(
        ((dy, dk) for dy in range(ny) for dk in range(CORES) if (dy, dk) != (0, 0)),
        key=lambda o: -(min(o[0], ny - o[0]) + 0.5 * o[1]))

    def col_at(dz, dx):
        return lax.rem(z + dz, nz) * NX + lax.rem(x + dx, NX)

    def row_at(dy, dk):
        return lax.rem(y + dy, ny) * CORES + lax.rem(core + dk, CORES)

    exists = [r < nrow - 1, r > 0, c < ncol - 1, c > 0]
    target = [(r + 1, c), (r - 1, c), (r, c + 1), (r, c - 1)]
    opposite = [1, 0, 3, 2]

    loads = [
        pltpu.make_async_copy(basis_hbm, basis, load_sem.at[0]),
        pltpu.make_async_copy(coarse_hbm, coarse, load_sem.at[1]),
        pltpu.make_async_copy(linv_hbm, linv, load_sem.at[2]),
        pltpu.make_async_copy(res_hbm, res_ref, load_sem.at[3]),
        pltpu.make_async_copy(ib_hbm, ib_ref, load_sem.at[4]),
        pltpu.make_async_copy(slots_hbm, slots_ref, load_sem.at[5]),
    ]
    for i in (3, 4, 0):
        loads[i].start()

    def line_x(dx):
        return (r, z * NX + lax.rem(x + dx, NX))

    def line_z(dz):
        return (r, lax.rem(z + dz, nz) * NX + x)

    across_x = [line_x(dx) for dx in (1, NX - 1, 2)]
    near_z = [line_z(dz) for dz in (1, nz - 1, 2, nz - 2)]
    up = jnp.logical_and(x == NX - 1, exists[2])
    down = jnp.logical_and(x == 0, exists[3])
    barrier = pltpu.get_barrier_semaphore()

    def signal(sem, device):
        pl.semaphore_signal(sem, inc=1, device_id=device, device_id_type=MESH)

    @pl.when(up)
    def _():
        signal(barrier, target[2])

    @pl.when(down)
    def _():
        signal(barrier, target[3])

    for offset in row_offsets:
        signal(barrier, (row_at(*offset), c))
    for device in across_x + near_z:
        signal(barrier, device)
    for i in (5, 1, 2):
        loads[i].start()
    loads[4].wait()
    loads[3].wait()

    blocks = [res_ref[:, b * BLK:(b + 1) * BLK] for b in range(own // BLK)]
    for d in range(4):
        index = ib_ref[0, d]
        value = blocks[0]
        for b in range(1, len(blocks)):
            value = jnp.where(index == b, blocks[b], value)
        outgoing[d] = value

        @pl.when(jnp.logical_not(exists[opposite[d]]))
        def _():
            incoming[d] = jnp.zeros_like(incoming[d])

        @pl.when(jnp.logical_not(exists[d]))
        def _():
            lent[d] = jnp.zeros_like(lent[d])

    def halo(d):
        return pltpu.make_async_remote_copy(
            src_ref=outgoing.at[d], dst_ref=incoming.at[d],
            send_sem=halo_send.at[d], recv_sem=halo_recv.at[d],
            device_id=target[d], device_id_type=MESH)

    def lend(d):
        return pltpu.make_async_remote_copy(
            src_ref=basis.at[:, pl.ds(own + d * BLK, BLK)], dst_ref=lent.at[d],
            send_sem=lend_send.at[d], recv_sem=lend_recv.at[d],
            device_id=target[opposite[d]], device_id_type=MESH)

    def send(phase, src, dst, device):
        pltpu.make_async_remote_copy(
            src_ref=src, dst_ref=dst, send_sem=bulk_send.at[phase], recv_sem=bulk_recv.at[phase],
            device_id=device, device_id_type=MESH).start()

    def arrived(phase, buf, count):
        some = buf.at[pl.ds(0, count)]
        pltpu.make_async_copy(some, some, bulk_recv.at[phase]).wait()

    def drained(phase, buf, count):
        some = buf.at[pl.ds(0, count)]
        pltpu.make_async_copy(some, some, bulk_send.at[phase]).wait()

    def spread_col(phase, buf, top, bot, ready):
        largest = jnp.maximum(jnp.abs(top), jnp.abs(bot))
        e, factor = scale_of(jnp.maximum(largest, half_roll(largest)))
        buf[c, :quarter] = to_words(top, bot, factor)
        buf[c, quarter:] = e[:1]
        ready()
        for offset in col_offsets:
            send(phase, buf.at[c], buf.at[c], (r, col_at(*offset)))

    def gathered(buf):
        columns = []
        for first in range(0, ncol, 2):
            a, b = buf[first, :quarter], buf[first + 1, :quarter]
            scale = scale_from(jnp.where(low1, buf[first, quarter:], buf[first + 1, quarter:]))
            quarters = from_words(jnp.where(low, a, half_roll(b))) + from_words(jnp.where(low, half_roll(a), b))
            columns.append(jnp.concatenate([v * scale for v in quarters], axis=0))
        return jnp.concatenate(split(jnp.concatenate(columns, axis=1)), axis=0)

    def largest_of(part):
        return functools.reduce(jnp.maximum, [jnp.abs(part[i:i + quarter]) for i in range(0, rhs, quarter)])

    def paired_words(part):
        e, factor = scale_of(largest_of(part))
        first = to_words(part[:quarter], part[quarter:half], factor)
        second = to_words(part[half:half + quarter], part[half + quarter:], factor)
        swapped = half_roll(e)
        return ((jnp.where(low, first, half_roll(second)), jnp.where(low, e, swapped)[:1]),
                (jnp.where(low, half_roll(first), second), jnp.where(low, swapped, e)[:1]))

    pl.semaphore_wait(barrier, nrow - 1 + len(across_x) + len(near_z) + up.astype(jnp.int32) + down.astype(jnp.int32))
    for d in range(4):
        @pl.when(exists[d])
        def _():
            halo(d).start()

    for device in across_x + near_z:
        signal(passed.at[0], device)
    loads[0].wait()
    b_hi, b_lo = split(basis[...])
    basis2[:nev] = b_hi
    basis2[nev:] = b_lo
    partial = matmul(res_ref[...], basis2[:, :own], NT)
    pl.semaphore_wait(passed.at[0], len(across_x) + len(near_z))
    for device in across_x:
        signal(passed.at[1], device)

    for d in range(4):
        @pl.when(exists[opposite[d]])
        def _():
            halo(d).wait_recv()

    inc = jnp.concatenate([incoming[d] for d in range(4)], axis=1)
    partial = partial + matmul(inc, basis2[:, own:], NT)
    partial = partial + half_roll(partial)
    spread_col(0, col1, jnp.where(low, partial[:quarter], partial[half:half + quarter]),
               jnp.where(low, partial[quarter:half], partial[half + quarter:]),
               lambda: pl.semaphore_wait(passed.at[1], len(across_x)))

    span = rows // nz
    loads[1].wait()
    for t in range(nz):
        at = slice(t * span, (t + 1) * span)
        coarse_t[:width, at], coarse_t[width:, at] = split(coarse[at].T)
    loads[2].wait()
    local = jnp.concatenate([res_ref[...], inc], axis=1)
    out_ref[...] = matmul(local, linv[...], NT)

    loads[5].wait()
    chunk = 2 * LANES
    place_in = lax.broadcasted_iota(jnp.int32, (width, chunk), 0) + c * width

    def build_in(i, carry):
        slot = slots_ref[:, pl.ds(pl.multiple_of(r * rows + i * chunk, chunk), chunk)]
        hot = jnp.where(place_in == slot, 1.0, 0.0).astype(BF16)
        hot_in[pl.ds(pl.multiple_of(i * chunk, chunk), chunk)] = hot.T
        return carry

    lax.fori_loop(0, rows // chunk, build_in, 0)

    arrived(0, col1, ncol - 1)
    part = matmul(gathered(col1), hot_in[...], NN)
    part = part[:rhs] + part[rhs:]
    blocks4 = width // LANES
    for q in range(blocks4):
        block = part[:, q * LANES:(q + 1) * LANES]
        e, factor = scale_of(largest_of(block))
        row1[r, q * half:(q + 1) * half] = to_words(block[:half], block[half:], factor[:1])
        row1[r, blocks4 * half + q:blocks4 * half + q + 1] = e[:1]
    for offset in row_offsets:
        send(1, row1.at[r], row1.at[r], (row_at(*offset), c))

    order = [(0, dy) for dy in range(ny)] + [(side, dy) for dy in far_first(ny) + [0] for side in (1, -1)]
    place = {key: i for i, key in enumerate(order)}
    low8 = lane_low((8, LANES))
    wanted = []
    for side, dy in order:
        safe = jnp.clip(c + side, 0, ncol - 1)
        first = lax.rem(y + dy, ny) * CORES * ncol + safe
        pair = []
        for device in (first, first + ncol):
            at = pl.ds(pl.multiple_of((device // 2) * LANES, LANES), LANES)
            pair.append(jnp.broadcast_to(slots_ref[:, at], (8, LANES)))
        even = jnp.where(low8, pair[0], half_roll(pair[1]))
        odd = jnp.where(low8, half_roll(pair[0]), pair[1])
        both = jnp.where(lax.rem(safe, 2) == 0, even, odd)[:1]
        if side:
            both = jnp.where(exists[2] if side > 0 else exists[3], both, -1)
        wanted.append(both)
    wanted = jnp.concatenate(wanted, axis=1) - r * rows
    place_out = lax.broadcasted_iota(jnp.int32, (LANES, wanted.shape[1]), 0)

    def build_out(i, carry):
        hot = jnp.where(place_out == wanted - i * LANES, 1.0, 0.0)
        hot_out[pl.ds(pl.multiple_of(i * LANES, LANES), LANES)] = hot.astype(BF16)
        return carry

    lax.fori_loop(0, rows // LANES, build_out, 0)

    arrived(1, row1, nrow - 1)
    column = []
    for q in range(blocks4):
        tops, bots = [], []
        for i in range(nrow):
            scale = scale_from(row1[i, blocks4 * half + q:blocks4 * half + q + 1])
            top, bot = from_words(row1[i, q * half:(q + 1) * half])
            tops.append(top * scale)
            bots.append(bot * scale)
        column.append(jnp.concatenate([tree_sum(tops), tree_sum(bots)], axis=0))
    column2 = jnp.concatenate(split(jnp.concatenate(column, axis=1)), axis=0)
    column4 = jnp.concatenate([column2, column2], axis=1)

    steps = far_first(nz) + [0]
    for batch in (steps[:2], steps[2:5], steps[5:]):
        parts = []
        for dz in batch:
            block = lax.rem(z + dz, nz)
            at = pl.ds(pl.multiple_of(block * span, span), span)
            part = matmul(column4, coarse_t[:, at], NN)
            parts.append((block, part[:rhs] + part[rhs:]))
        for block, part in parts:
            for q in range(span // LANES):
                for i, (words, e) in enumerate(paired_words(part[:, q * LANES:(q + 1) * LANES])):
                    pieces[block * NX + 2 * q + i, :quarter] = words
                    pieces[block * NX + 2 * q + i, quarter:] = e
        for dz, (block, part) in zip(batch, parts):
            for dx in (2, 1, 3, 0) if dz else (2, 1, 3):
                to = block * NX + lax.rem(x + dx, NX)
                send(2, pieces.at[to], received.at[c], (r, to))

    for d in range(4):
        @pl.when(exists[opposite[d]])
        def _():
            lend(d).start()

    received[c] = pieces[c]
    arrived(2, received, ncol - 1)
    tops, bots = [], []
    for i in range(ncol):
        scale = scale_from(received[i, quarter:])
        top, bot = from_words(received[i, :quarter])
        tops.append(top * scale)
        bots.append(bot * scale)
    top, bot = tree_sum(tops), tree_sum(bots)
    spread_col(3, col2, top, bot, lambda: None)

    wide_hi[:nev] = basis2[:nev, :own]
    wide_lo[:nev] = basis2[nev:, :own]
    wide_hi[5 * nev:] = jnp.zeros_like(wide_hi[5 * nev:])
    wide_lo[5 * nev:] = jnp.zeros_like(wide_lo[5 * nev:])
    for d in range(4):
        @pl.when(exists[d])
        def _():
            lend(d).wait_recv()

        l_hi, l_lo = split(lent[d])
        for b in range(own // BLK):
            here = ib_ref[0, d] == b
            at = slice((d + 1) * nev, (d + 2) * nev), slice(b * BLK, (b + 1) * BLK)
            wide_hi[at] = jnp.where(here, l_hi, jnp.zeros_like(l_hi))
            wide_lo[at] = jnp.where(here, l_lo, jnp.zeros_like(l_lo))

    arrived(3, col2, ncol - 1)
    solution = gathered(col2)
    groups = []
    for dys, stop in (((2,), ny + 2), ((1, 3), ny + 6), ((0,), ny + 8)):
        start = len(groups) // 2
        part = matmul(solution, hot_out[:, start * LANES:stop * LANES], NN)
        part = part[:rhs] + part[rhs:]
        for q in range(stop - start):
            groups.extend(paired_words(part[:, q * LANES:(q + 1) * LANES]))
        for dy in dys:
            for k in range(CORES):
                up_row = (0, (dy + (k + 1) // CORES) % ny, (k + 1) % CORES)
                down_row = (0, (dy + (k - 1) // CORES) % ny, (k - 1) % CORES)
                to = lax.rem(y + dy, ny) * CORES + k
                for i, (side, at_y, at_k) in enumerate(((0, dy, k), up_row, down_row, (1, dy, k), (-1, dy, k))):
                    words, e = groups[2 * place[side, at_y] + at_k]
                    sets[to, i * quarter:(i + 1) * quarter] = words
                    sets[to, 5 * quarter + i:5 * quarter + i + 1] = e
            if dy:
                for dk in range(CORES):
                    to = row_at(dy, dk)
                    send(4, sets.at[to], row2.at[r], (to, c))
            else:
                to = row_at(0, 1)
                send(4, sets.at[to], row2.at[r], (to, c))
    row2[r] = sets[r]
    arrived(4, row2, nrow - 1)
    picks = []
    for k in range(5):
        tops, bots = [], []
        for i in range(nrow):
            scale = scale_from(row2[i, 5 * quarter + k:5 * quarter + k + 1])
            top, bot = from_words(row2[i, k * quarter:(k + 1) * quarter])
            tops.append(top * scale)
            bots.append(bot * scale)
        picks.append((tree_sum(tops), tree_sum(bots)))
    picks.append((jnp.zeros_like(picks[0][0]),) * 2)
    columns = []
    for p in range(3):
        a, b = picks[2 * p], picks[2 * p + 1]
        columns.append(jnp.concatenate(
            [jnp.where(low, a[i], half_roll(b[i])) for i in range(2)]
            + [jnp.where(low, half_roll(a[i]), b[i]) for i in range(2)], axis=0))
    picked = jnp.concatenate(split(jnp.concatenate(columns, axis=1)), axis=0)
    inner = matmul(picked, wide_hi[...], NN) + matmul(picked, wide_lo[...], NN)
    out_ref[...] = out_ref[...] + inner[:rhs] + inner[rhs:]

    drained(0, col1, ncol - 1)
    drained(1, row1, nrow - 1)
    drained(2, received, ncol - 1)
    drained(3, col2, ncol - 1)
    drained(4, row2, nrow - 1)
    for d in range(4):
        @pl.when(exists[d])
        def _():
            halo(d).wait_send()

        @pl.when(exists[opposite[d]])
        def _():
            lend(d).wait_send()


def shards(nrow, ncol, residuals, intersect_blocks, local_inverse, coarse_basis, coarse_slots, coarse_inverse):
    own, rhs = residuals.shape
    loc, nev = coarse_basis.shape
    rows, width = coarse_inverse.shape
    total = coarse_slots.shape[0]
    assert 2 * nev == LANES and rows == ncol * nev and width == nrow * nev and loc == own + 4 * BLK and own % BLK == 0
    vmem = pl.BlockSpec(memory_space=pltpu.VMEM)
    hbm = pl.BlockSpec(memory_space=pl.ANY)
    dma = pltpu.SemaphoreType.DMA
    out = pl.pallas_call(
        functools.partial(kernel, nrow, ncol),
        name="schwarz",
        out_shape=pltpu.VMEM((rhs, own), F32),
        in_specs=[hbm] * 6,
        out_specs=vmem,
        scratch_shapes=[
            pltpu.VMEM((rhs, own), BF16),
            pltpu.SMEM(intersect_blocks.shape, jnp.int32),
            pltpu.VMEM((1, total), jnp.int32),
            pltpu.VMEM((4, rhs, BLK), BF16),
            pltpu.VMEM((4, rhs, BLK), BF16),
            pltpu.VMEM((own, loc), BF16),
            pltpu.VMEM((nev, loc), F32),
            pltpu.VMEM((2 * nev, loc), BF16),
            pltpu.VMEM((rows, width), F32),
            pltpu.VMEM((2 * width, rows), BF16),
            pltpu.VMEM((rows, width), BF16),
            pltpu.VMEM((rows, 3 * width), BF16),
            pltpu.VMEM((ncol, rhs // 4 + 1, LANES), jnp.int32),
            pltpu.VMEM((nrow, width // LANES * (rhs // 2 + 1), LANES), jnp.int32),
            pltpu.VMEM((ncol, rhs // 4 + 1, LANES), jnp.int32),
            pltpu.VMEM((ncol, rhs // 4 + 1, LANES), jnp.int32),
            pltpu.VMEM((ncol, rhs // 4 + 1, LANES), jnp.int32),
            pltpu.VMEM((nrow, 5 * (rhs // 4 + 1), LANES), jnp.int32),
            pltpu.VMEM((nrow, 5 * (rhs // 4 + 1), LANES), jnp.int32),
            pltpu.VMEM((4, nev, BLK), F32),
            pltpu.VMEM((6 * nev, own), BF16),
            pltpu.VMEM((6 * nev, own), BF16),
            dma((6,)),
            dma((4,)),
            dma((4,)),
            dma((4,)),
            dma((4,)),
            dma((5,)),
            dma((5,)),
            pltpu.SemaphoreType.REGULAR((2,)),
        ],
        compiler_params=pltpu.CompilerParams(collective_id=0, has_side_effects=True),
    )(
        residuals.T,
        intersect_blocks,
        local_inverse,
        coarse_basis.T,
        coarse_slots.reshape(1, total),
        coarse_inverse,
    )
    return out.T


def solution(mesh):
    placed = (
        P(("row", "col"), None),
        P(("row", "col"), None),
        P(("row", "col"), None),
        P(("row", "col"), None),
        P(),
        P("row", "col"),
    )
    return jax.shard_map(
        functools.partial(shards, mesh.shape["row"], mesh.shape["col"]),
        mesh=mesh, in_specs=placed, out_specs=P(("row", "col"), None), check_vma=False,
    )
```

```python
import functools

import jax
import jax.numpy as jnp
from jax import lax
from jax.experimental import pallas as pl
from jax.experimental.pallas import tpu as pltpu
from jax.sharding import PartitionSpec as P

MESH = pl.DeviceIdType.MESH
BLK = 128
LANES = 128
NX = 4
CORES = 2
PEAK = 32760.0
STEPS = 8.0
TINY = 1e-30
NT = (((1,), (1,)), ((), ()))
NN = (((1,), (0,)), ((), ()))
F32 = jnp.float32
BF16 = jnp.bfloat16


def matmul(a, b, dims):
    return lax.dot_general(a, b, dims, preferred_element_type=F32)


def split(x):
    hi = x.astype(BF16)
    return hi, (x - hi.astype(F32)).astype(BF16)


def lane_low(shape):
    return lax.broadcasted_iota(jnp.int32, shape, len(shape) - 1) < LANES // 2


def half_roll(x):
    return pltpu.roll(x, LANES // 2, 1)


def far_first(count):
    return sorted(range(1, count), key=lambda k: -min(k, count - k))


def tree_sum(parts):
    while len(parts) > 1:
        parts = [parts[i] + parts[i + 1] if i + 1 < len(parts) else parts[i] for i in range(0, len(parts), 2)]
    return parts[0]


def scale_of(largest):
    top = jnp.broadcast_to(jnp.max(largest, axis=0, keepdims=True), largest.shape)
    e = jnp.ceil(jnp.log2(jnp.maximum(top, TINY)) * STEPS)
    return e.astype(jnp.int32), jnp.exp2(e * (-1.0 / STEPS)) * PEAK


def scale_from(row):
    return jnp.exp2(row.astype(F32) * (1.0 / STEPS)) * (1.0 / PEAK)


def to_words(top, bot, factor):
    a = jnp.round(top * factor).astype(jnp.int32)
    b = jnp.round(bot * factor).astype(jnp.int32)
    return (a << 16) | (b & 0xFFFF)


def from_words(w):
    return (w >> 16).astype(F32), ((w << 16) >> 16).astype(F32)


def kernel(
    nrow,
    ncol,
    res_hbm,
    ib_hbm,
    linv_hbm,
    basis_hbm,
    slots_hbm,
    coarse_hbm,
    out_ref,
    res_ref,
    ib_ref,
    slots_ref,
    outgoing,
    incoming,
    linv,
    basis,
    basis2,
    coarse,
    coarse_t,
    hot_in,
    hot_out,
    col1,
    row1,
    product,
    pieces,
    received,
    col2,
    sets,
    row2,
    lent,
    wide,
    load_sem,
    sent,
    halo_recv,
    lend_recv,
    bulk_recv,
    passed,
):
    r = lax.axis_index("row")
    c = lax.axis_index("col")
    z, x = c // NX, lax.rem(c, NX)
    y, core = r // CORES, lax.rem(r, CORES)
    nz, ny = ncol // NX, nrow // CORES
    rhs = res_ref.shape[0]
    own = res_ref.shape[1]
    half = rhs // 2
    quarter = rhs // 4
    rows, width = coarse.shape
    nev = basis.shape[0]
    low = lane_low((quarter, LANES))
    low1 = lane_low((1, LANES))

    col_offsets = sorted(
        ((dz, dx) for dz in range(nz) for dx in range(NX) if (dz, dx) != (0, 0)),
        key=lambda o: -(min(o[0], nz - o[0]) + min(o[1], NX - o[1])))
    row_offsets = sorted(
        ((dy, dk) for dy in range(ny) for dk in range(CORES) if (dy, dk) != (0, 0)),
        key=lambda o: -(min(o[0], ny - o[0]) + 0.5 * o[1]))

    def col_at(dz, dx):
        return lax.rem(z + dz, nz) * NX + lax.rem(x + dx, NX)

    def row_at(dy, dk):
        return lax.rem(y + dy, ny) * CORES + lax.rem(core + dk, CORES)

    exists = [r < nrow - 1, r > 0, c < ncol - 1, c > 0]
    target = [(r + 1, c), (r - 1, c), (r, c + 1), (r, c - 1)]
    opposite = [1, 0, 3, 2]

    loads = [
        pltpu.make_async_copy(basis_hbm, basis, load_sem.at[0]),
        pltpu.make_async_copy(coarse_hbm, coarse, load_sem.at[1]),
        pltpu.make_async_copy(linv_hbm, linv, load_sem.at[2]),
        pltpu.make_async_copy(res_hbm, res_ref, load_sem.at[3]),
        pltpu.make_async_copy(ib_hbm, ib_ref, load_sem.at[4]),
        pltpu.make_async_copy(slots_hbm, slots_ref, load_sem.at[5]),
    ]
    for i in (3, 4, 0):
        loads[i].start()

    def line_x(dx):
        return (r, z * NX + lax.rem(x + dx, NX))

    def line_z(dz):
        return (r, lax.rem(z + dz, nz) * NX + x)

    across_x = [line_x(dx) for dx in far_first(NX)]
    near_z = [line_z(dz) for dz in (2, nz - 2, 1, nz - 1)]
    greeted = across_x + near_z
    up = jnp.logical_and(x == NX - 1, exists[2])
    down = jnp.logical_and(x == 0, exists[3])
    barrier = pltpu.get_barrier_semaphore()

    def signal(sem, device):
        pl.semaphore_signal(sem, inc=1, device_id=device, device_id_type=MESH)

    @pl.when(up)
    def _():
        signal(barrier, target[2])

    @pl.when(down)
    def _():
        signal(barrier, target[3])

    for offset in row_offsets:
        signal(barrier, (row_at(*offset), c))
    for device in greeted:
        signal(barrier, device)
    for i in (5, 1, 2):
        loads[i].start()
    loads[4].wait()
    loads[3].wait()

    blocks = [res_ref[:, b * BLK:(b + 1) * BLK] for b in range(own // BLK)]
    for d in range(4):
        index = ib_ref[0, d]
        value = blocks[0]
        for b in range(1, len(blocks)):
            value = jnp.where(index == b, blocks[b], value)
        outgoing[d] = value

        @pl.when(jnp.logical_not(exists[opposite[d]]))
        def _():
            incoming[d] = jnp.zeros_like(incoming[d])

        @pl.when(jnp.logical_not(exists[d]))
        def _():
            lent[d] = jnp.zeros_like(lent[d])

    def halo(d):
        return pltpu.make_async_remote_copy(
            src_ref=outgoing.at[d], dst_ref=incoming.at[d],
            send_sem=sent.at[0], recv_sem=halo_recv.at[d],
            device_id=target[d], device_id_type=MESH)

    def lend(d):
        return pltpu.make_async_remote_copy(
            src_ref=basis.at[:, pl.ds(own + d * BLK, BLK)], dst_ref=lent.at[d],
            send_sem=sent.at[0], recv_sem=lend_recv.at[d],
            device_id=target[opposite[d]], device_id_type=MESH)

    def send(phase, src, dst, device):
        pltpu.make_async_remote_copy(
            src_ref=src, dst_ref=dst, send_sem=sent.at[0], recv_sem=bulk_recv.at[phase],
            device_id=device, device_id_type=MESH).start()

    def arrived(phase, buf, count):
        some = buf.at[pl.ds(0, count)]
        pltpu.make_async_copy(some, some, bulk_recv.at[phase]).wait()

    def drained(buf, count):
        some = buf.at[pl.ds(0, count)]
        pltpu.make_async_copy(some, some, sent.at[0]).wait()

    def spread_col(phase, buf, top, bot, ready):
        largest = jnp.maximum(jnp.abs(top), jnp.abs(bot))
        e, factor = scale_of(jnp.maximum(largest, half_roll(largest)))
        buf[c, :quarter] = to_words(top, bot, factor)
        buf[c, quarter:] = e[:1]
        ready()
        for offset in col_offsets:
            send(phase, buf.at[c], buf.at[c], (r, col_at(*offset)))

    def gathered(buf):
        columns = []
        for first in range(0, ncol, 2):
            a, b = buf[first, :quarter], buf[first + 1, :quarter]
            scale = scale_from(jnp.where(low1, buf[first, quarter:], buf[first + 1, quarter:]))
            quarters = from_words(jnp.where(low, a, half_roll(b))) + from_words(jnp.where(low, half_roll(a), b))
            columns.append(jnp.concatenate([v * scale for v in quarters], axis=0))
        return jnp.concatenate(split(jnp.concatenate(columns, axis=1)), axis=0)

    def largest_of(part):
        return functools.reduce(jnp.maximum, [jnp.abs(part[i:i + quarter]) for i in range(0, rhs, quarter)])

    def paired_words(part):
        e, factor = scale_of(largest_of(part))
        first = to_words(part[:quarter], part[quarter:half], factor)
        second = to_words(part[half:half + quarter], part[half + quarter:], factor)
        swapped = half_roll(e)
        return ((jnp.where(low, first, half_roll(second)), jnp.where(low, e, swapped)[:1]),
                (jnp.where(low, half_roll(first), second), jnp.where(low, swapped, e)[:1]))

    pl.semaphore_wait(barrier, nrow - 1 + len(greeted) + up.astype(jnp.int32) + down.astype(jnp.int32))
    for d in range(4):
        @pl.when(exists[d])
        def _():
            halo(d).start()

    for device in greeted:
        signal(passed.at[0], device)
    loads[0].wait()
    b_hi, b_lo = split(basis[...])
    basis2[:nev] = b_hi
    basis2[nev:] = b_lo
    partial = matmul(res_ref[...], basis2[:, :own], NT)

    pl.semaphore_wait(passed.at[0], len(greeted))
    for device in across_x:
        signal(passed.at[1], device)
    for d in range(4):
        @pl.when(exists[opposite[d]])
        def _():
            halo(d).wait_recv()

    inc = jnp.concatenate([incoming[d] for d in range(4)], axis=1)
    partial = partial + matmul(inc, basis2[:, own:], NT)
    partial = partial + half_roll(partial)
    spread_col(0, col1, jnp.where(low, partial[:quarter], partial[half:half + quarter]),
               jnp.where(low, partial[quarter:half], partial[half + quarter:]),
               lambda: pl.semaphore_wait(passed.at[1], NX - 1))

    span = rows // nz
    loads[1].wait()
    for t in range(nz):
        at = slice(t * span, (t + 1) * span)
        for h in range(2):
            turned = split(coarse[at, h * (width // 2):(h + 1) * (width // 2)].T)
            coarse_t[h * width:h * width + width // 2, at], coarse_t[h * width + width // 2:(h + 1) * width, at] = turned
    loads[2].wait()
    local = jnp.concatenate([res_ref[...], inc], axis=1)
    out_ref[...] = matmul(local, linv[...], NT)

    loads[5].wait()
    chunk = 2 * LANES
    place_in = lax.broadcasted_iota(jnp.int32, (width, chunk), 0) + c * width

    def build_in(i, carry):
        slot = slots_ref[:, pl.ds(pl.multiple_of(r * rows + i * chunk, chunk), chunk)]
        hot = jnp.where(place_in == slot, 1.0, 0.0).astype(BF16)
        hot_in[pl.ds(pl.multiple_of(i * chunk, chunk), chunk)] = hot.T
        return carry

    lax.fori_loop(0, rows // chunk, build_in, 0)

    arrived(0, col1, ncol - 1)
    partials = gathered(col1)
    part_blocks = width // 2 // LANES
    for h in range(2):
        part = matmul(partials, hot_in[:, h * (width // 2):(h + 1) * (width // 2)], NN)
        part = part[:rhs] + part[rhs:]
        for q in range(part_blocks):
            block = part[:, q * LANES:(q + 1) * LANES]
            e, factor = scale_of(largest_of(block))
            row1[h, r, q * half:(q + 1) * half] = to_words(block[:half], block[half:], factor[:1])
            row1[h, r, part_blocks * half + q:part_blocks * half + q + 1] = e[:1]
        for offset in row_offsets:
            send(1 + h, row1.at[h, r], row1.at[h, r], (row_at(*offset), c))

    def sides(dy):
        return [((side, dy, 0), (side, dy, 1)) for side in (1, -1)]

    order = [((0, 2, 0), (0, 2, 1)), ((0, 3, 0), (0, 1, 1))] + sides(2)
    order += [((0, 1, 0), (0, 3, 1)), ((0, 0, 0), (0, 0, 1))] + sides(1) + sides(3) + sides(0)
    place = {key: 2 * i + j for i, pair in enumerate(order) for j, key in enumerate(pair)}
    wanted = []
    for keys in order:
        side = keys[0][0]
        safe = jnp.clip(c + side, 0, ncol - 1)
        pair = []
        for _, dy, k in keys:
            device = (lax.rem(y + dy, ny) * CORES + k) * ncol + safe
            at = pl.ds(pl.multiple_of((device // 2) * LANES, LANES), LANES)
            pair.append(jnp.broadcast_to(slots_ref[:, at], (8, LANES)))
        even = jnp.where(low, pair[0], half_roll(pair[1]))
        odd = jnp.where(low, half_roll(pair[0]), pair[1])
        both = jnp.where(lax.rem(safe, 2) == 0, even, odd)[:1]
        if side:
            both = jnp.where(exists[2] if side > 0 else exists[3], both, -1)
        wanted.append(both)
    wanted = jnp.concatenate(wanted, axis=1) - r * rows
    place_out = lax.broadcasted_iota(jnp.int32, (LANES, wanted.shape[1]), 0)

    def build_out(i, carry):
        hot = jnp.where(place_out == wanted - i * LANES, 1.0, 0.0)
        hot_out[pl.ds(pl.multiple_of(i * LANES, LANES), LANES)] = hot.astype(BF16)
        return carry

    lax.fori_loop(0, rows // LANES, build_out, 0)

    def column_half(h):
        arrived(1 + h, row1.at[h], nrow - 1)
        column = []
        for q in range(part_blocks):
            tops, bots = [], []
            for i in range(nrow):
                scale = scale_from(row1[h, i, part_blocks * half + q:part_blocks * half + q + 1])
                top, bot = from_words(row1[h, i, q * half:(q + 1) * half])
                tops.append(top * scale)
                bots.append(bot * scale)
            column.append(jnp.concatenate([tree_sum(tops), tree_sum(bots)], axis=0))
        value = jnp.concatenate(split(jnp.concatenate(column, axis=1)), axis=0)
        return jnp.concatenate([value, value], axis=1)

    first_half = column_half(0)
    for t in range(nz):
        at = slice(t * span, (t + 1) * span)
        part = matmul(first_half, coarse_t[:width, at], NN)
        product[:, at] = part[:rhs] + part[rhs:]
    second_half = column_half(1)
    steps = far_first(nz) + [0]
    for batch in (steps[:2], steps[2:5], steps[5:]):
        parts = []
        for dz in batch:
            block = lax.rem(z + dz, nz)
            at = pl.ds(pl.multiple_of(block * span, span), span)
            part = matmul(second_half, coarse_t[width:, at], NN)
            parts.append((block, part[:rhs] + part[rhs:] + product[:, at]))
        for block, part in parts:
            for q in range(span // LANES):
                for i, (words, e) in enumerate(paired_words(part[:, q * LANES:(q + 1) * LANES])):
                    pieces[block * NX + 2 * q + i, :quarter] = words
                    pieces[block * NX + 2 * q + i, quarter:] = e
        for dz, (block, part) in zip(batch, parts):
            for dx in (2, 1, 3, 0) if dz else (2, 1, 3):
                to = block * NX + lax.rem(x + dx, NX)
                send(3, pieces.at[to], received.at[c], (r, to))

    for d in range(4):
        @pl.when(exists[opposite[d]])
        def _():
            lend(d).start()

    received[c] = pieces[c]
    arrived(3, received, ncol - 1)
    tops, bots = [], []
    for i in range(ncol):
        scale = scale_from(received[i, quarter:])
        top, bot = from_words(received[i, :quarter])
        tops.append(top * scale)
        bots.append(bot * scale)
    top, bot = tree_sum(tops), tree_sum(bots)
    spread_col(4, col2, top, bot, lambda: None)

    wide[:nev] = basis2[:nev, :own]
    wide[6 * nev:7 * nev] = basis2[nev:, :own]
    for at in (5 * nev, 11 * nev):
        wide[at:at + nev] = jnp.zeros_like(wide[at:at + nev])
    for d in range(4):
        @pl.when(exists[d])
        def _():
            lend(d).wait_recv()

        l_hi, l_lo = split(lent[d])
        for b in range(own // BLK):
            here = ib_ref[0, d] == b
            at = slice(b * BLK, (b + 1) * BLK)
            wide[(d + 1) * nev:(d + 2) * nev, at] = jnp.where(here, l_hi, jnp.zeros_like(l_hi))
            wide[(d + 7) * nev:(d + 8) * nev, at] = jnp.where(here, l_lo, jnp.zeros_like(l_lo))

    arrived(4, col2, ncol - 1)
    solution = gathered(col2)
    groups = []
    for dys, stop in (((2,), 4), ((1, 3), 10), ((0,), 12)):
        start = len(groups) // 2
        part = matmul(solution, hot_out[:, start * LANES:stop * LANES], NN)
        part = part[:rhs] + part[rhs:]
        for q in range(stop - start):
            groups.extend(paired_words(part[:, q * LANES:(q + 1) * LANES]))
        for dy in dys:
            for k in range(CORES):
                up_row = (0, (dy + (k + 1) // CORES) % ny, (k + 1) % CORES)
                down_row = (0, (dy + (k - 1) // CORES) % ny, (k - 1) % CORES)
                to = lax.rem(y + dy, ny) * CORES + k
                for i, (side, at_y, at_k) in enumerate(((0, dy, k), up_row, down_row, (1, dy, k), (-1, dy, k))):
                    words, e = groups[place[side, at_y, at_k]]
                    sets[to, i * quarter:(i + 1) * quarter] = words
                    sets[to, 5 * quarter + i:5 * quarter + i + 1] = e
            if dy:
                for dk in range(CORES):
                    to = row_at(dy, dk)
                    send(5, sets.at[to], row2.at[r], (to, c))
            else:
                to = row_at(0, 1)
                send(5, sets.at[to], row2.at[r], (to, c))
    row2[r] = sets[r]
    arrived(5, row2, nrow - 1)
    picks = []
    for k in range(5):
        tops, bots = [], []
        for i in range(nrow):
            scale = scale_from(row2[i, 5 * quarter + k:5 * quarter + k + 1])
            top, bot = from_words(row2[i, k * quarter:(k + 1) * quarter])
            tops.append(top * scale)
            bots.append(bot * scale)
        picks.append((tree_sum(tops), tree_sum(bots)))
    picks.append((jnp.zeros_like(picks[0][0]),) * 2)
    columns = []
    for p in range(3):
        a, b = picks[2 * p], picks[2 * p + 1]
        columns.append(jnp.concatenate(
            [jnp.where(low, a[i], half_roll(b[i])) for i in range(2)]
            + [jnp.where(low, half_roll(a[i]), b[i]) for i in range(2)], axis=0))
    picked = jnp.concatenate(split(jnp.concatenate(columns, axis=1)), axis=0)
    inner = matmul(jnp.concatenate([picked, picked], axis=1), wide[...], NN)
    out_ref[...] = out_ref[...] + inner[:rhs] + inner[rhs:]

    drained(col1, ncol - 1)
    drained(row1.at[0], nrow - 1)
    drained(row1.at[1], nrow - 1)
    drained(received, ncol - 1)
    drained(col2, ncol - 1)
    drained(row2, nrow - 1)
    for d in range(4):
        @pl.when(exists[d])
        def _():
            halo(d).wait_send()

        @pl.when(exists[opposite[d]])
        def _():
            lend(d).wait_send()


def shards(nrow, ncol, residuals, intersect_blocks, local_inverse, coarse_basis, coarse_slots, coarse_inverse):
    own, rhs = residuals.shape
    loc, nev = coarse_basis.shape
    rows, width = coarse_inverse.shape
    total = coarse_slots.shape[0]
    assert 2 * nev == LANES and rows == ncol * nev and width == nrow * nev and loc == own + 4 * BLK and own % BLK == 0
    vmem = pl.BlockSpec(memory_space=pltpu.VMEM)
    hbm = pl.BlockSpec(memory_space=pl.ANY)
    dma = pltpu.SemaphoreType.DMA
    out = pl.pallas_call(
        functools.partial(kernel, nrow, ncol),
        name="schwarz",
        out_shape=pltpu.VMEM((rhs, own), F32),
        in_specs=[hbm] * 6,
        out_specs=vmem,
        scratch_shapes=[
            pltpu.VMEM((rhs, own), BF16),
            pltpu.SMEM(intersect_blocks.shape, jnp.int32),
            pltpu.VMEM((1, total), jnp.int32),
            pltpu.VMEM((4, rhs, BLK), BF16),
            pltpu.VMEM((4, rhs, BLK), BF16),
            pltpu.VMEM((own, loc), BF16),
            pltpu.VMEM((nev, loc), F32),
            pltpu.VMEM((2 * nev, loc), BF16),
            pltpu.VMEM((rows, width), F32),
            pltpu.VMEM((2 * width, rows), BF16),
            pltpu.VMEM((rows, width), BF16),
            pltpu.VMEM((rows, 3 * width), BF16),
            pltpu.VMEM((ncol, rhs // 4 + 1, LANES), jnp.int32),
            pltpu.VMEM((2, nrow, width // 2 // LANES * (rhs // 2 + 1), LANES), jnp.int32),
            pltpu.VMEM((rhs, rows), F32),
            pltpu.VMEM((ncol, rhs // 4 + 1, LANES), jnp.int32),
            pltpu.VMEM((ncol, rhs // 4 + 1, LANES), jnp.int32),
            pltpu.VMEM((ncol, rhs // 4 + 1, LANES), jnp.int32),
            pltpu.VMEM((nrow, 5 * (rhs // 4 + 1), LANES), jnp.int32),
            pltpu.VMEM((nrow, 5 * (rhs // 4 + 1), LANES), jnp.int32),
            pltpu.VMEM((4, nev, BLK), F32),
            pltpu.VMEM((12 * nev, own), BF16),
            dma((6,)),
            dma((1,)),
            dma((4,)),
            dma((4,)),
            dma((6,)),
            pltpu.SemaphoreType.REGULAR((2,)),
        ],
        compiler_params=pltpu.CompilerParams(collective_id=0, has_side_effects=True),
    )(
        residuals.T,
        intersect_blocks,
        local_inverse,
        coarse_basis.T,
        coarse_slots.reshape(1, total),
        coarse_inverse,
    )
    return out.T


def solution(mesh):
    placed = (
        P(("row", "col"), None),
        P(("row", "col"), None),
        P(("row", "col"), None),
        P(("row", "col"), None),
        P(),
        P("row", "col"),
    )
    return jax.shard_map(
        functools.partial(shards, mesh.shape["row"], mesh.shape["col"]),
        mesh=mesh, in_specs=placed, out_specs=P(("row", "col"), None), check_vma=False,
    )
```

```python
import functools

import jax
import jax.numpy as jnp
from jax import lax
from jax.experimental import pallas as pl
from jax.experimental.pallas import tpu as pltpu
from jax.sharding import PartitionSpec as P

MESH = pl.DeviceIdType.MESH
BLK = 128
LANES = 128
NX = 4
CORES = 2
PEAK = 32760.0
TINY = 1e-30
NT = (((1,), (1,)), ((), ()))
NN = (((1,), (0,)), ((), ()))
F32 = jnp.float32
BF16 = jnp.bfloat16


def matmul(a, b, dims):
    return lax.dot_general(a, b, dims, preferred_element_type=F32)


def split(x):
    hi = x.astype(BF16)
    return hi, (x - hi.astype(F32)).astype(BF16)


def lane_low(shape):
    return lax.broadcasted_iota(jnp.int32, shape, len(shape) - 1) < LANES // 2


def half_roll(x):
    return pltpu.roll(x, LANES // 2, 1)


def far_first(count):
    return sorted(range(1, count), key=lambda k: -min(k, count - k))


def tree_sum(parts):
    while len(parts) > 1:
        parts = [parts[i] + parts[i + 1] if i + 1 < len(parts) else parts[i] for i in range(0, len(parts), 2)]
    return parts[0]


def scale_of(largest):
    top = jnp.broadcast_to(jnp.max(largest, axis=0, keepdims=True), largest.shape)
    e = jnp.ceil(jnp.log2(jnp.maximum(top, TINY)))
    return e.astype(jnp.int32), jnp.exp2(-e) * PEAK


def scale_from(row):
    return jnp.exp2(row.astype(F32)) * (1.0 / PEAK)


def to_words(top, bot, factor):
    a = jnp.round(top * factor).astype(jnp.int32)
    b = jnp.round(bot * factor).astype(jnp.int32)
    return pack(a, b)


def pack(top, bot):
    return (top << 16) | (bot & 0xFFFF)


def from_words(w):
    return (w >> 16).astype(F32), ((w << 16) >> 16).astype(F32)


def kernel(
    nrow,
    ncol,
    res_hbm,
    ib_hbm,
    linv_hbm,
    basis_hbm,
    slots_hbm,
    coarse_hbm,
    out_ref,
    res_ref,
    ib_ref,
    slots_ref,
    outgoing,
    incoming,
    linv,
    basis,
    basis2,
    coarse,
    coarse_t,
    hot_in,
    hot_out,
    col1,
    row1,
    product,
    pieces,
    received,
    col2,
    sets,
    row2,
    lent,
    wide,
    load_sem,
    sent,
    halo_recv,
    lend_recv,
    bulk_recv,
    passed,
):
    r = lax.axis_index("row")
    c = lax.axis_index("col")
    z, x = c // NX, lax.rem(c, NX)
    y, core = r // CORES, lax.rem(r, CORES)
    nz, ny = ncol // NX, nrow // CORES
    rhs = res_ref.shape[0]
    own = res_ref.shape[1]
    half = rhs // 2
    quarter = rhs // 4
    rows, width = coarse.shape
    nev = basis.shape[0]
    low = lane_low((quarter, LANES))
    low1 = lane_low((1, LANES))

    col_offsets = sorted(
        ((dz, dx) for dz in range(nz) for dx in range(NX) if (dz, dx) != (0, 0)),
        key=lambda o: -(min(o[0], nz - o[0]) + min(o[1], NX - o[1])))
    row_offsets = sorted(
        ((dy, dk) for dy in range(ny) for dk in range(CORES) if (dy, dk) != (0, 0)),
        key=lambda o: -(min(o[0], ny - o[0]) + 0.5 * o[1]))

    origin_first = sorted(range(ncol), key=lambda i: min(i // NX, nz - i // NX) + min(i % NX, NX - i % NX))

    def col_at(dz, dx):
        return lax.rem(z + dz, nz) * NX + lax.rem(x + dx, NX)

    def row_at(dy, dk):
        return lax.rem(y + dy, ny) * CORES + lax.rem(core + dk, CORES)

    exists = [r < nrow - 1, r > 0, c < ncol - 1, c > 0]
    target = [(r + 1, c), (r - 1, c), (r, c + 1), (r, c - 1)]
    opposite = [1, 0, 3, 2]

    loads = [
        pltpu.make_async_copy(basis_hbm, basis, load_sem.at[0]),
        pltpu.make_async_copy(coarse_hbm, coarse, load_sem.at[1]),
        pltpu.make_async_copy(linv_hbm, linv, load_sem.at[2]),
        pltpu.make_async_copy(res_hbm, res_ref, load_sem.at[3]),
        pltpu.make_async_copy(ib_hbm, ib_ref, load_sem.at[4]),
        pltpu.make_async_copy(slots_hbm, slots_ref, load_sem.at[5]),
    ]
    for i in (3, 4, 0):
        loads[i].start()

    def line_x(dx):
        return (r, z * NX + lax.rem(x + dx, NX))

    def line_z(dz):
        return (r, lax.rem(z + dz, nz) * NX + x)

    across_x = [line_x(dx) for dx in far_first(NX)]
    near_z = [line_z(dz) for dz in (2, nz - 2, 1, nz - 1)]
    greeted = across_x + near_z
    up = jnp.logical_and(x == NX - 1, exists[2])
    down = jnp.logical_and(x == 0, exists[3])
    barrier = pltpu.get_barrier_semaphore()

    def signal(sem, device):
        pl.semaphore_signal(sem, inc=1, device_id=device, device_id_type=MESH)

    @pl.when(up)
    def _():
        signal(barrier, target[2])

    @pl.when(down)
    def _():
        signal(barrier, target[3])

    for offset in row_offsets:
        signal(barrier, (row_at(*offset), c))
    for device in greeted:
        signal(barrier, device)
    for i in (5, 1, 2):
        loads[i].start()
    loads[4].wait()
    loads[3].wait()

    blocks = [res_ref[:, b * BLK:(b + 1) * BLK] for b in range(own // BLK)]
    for d in range(4):
        index = ib_ref[0, d]
        value = blocks[0]
        for b in range(1, len(blocks)):
            value = jnp.where(index == b, blocks[b], value)
        outgoing[d] = value

        @pl.when(jnp.logical_not(exists[opposite[d]]))
        def _():
            incoming[d] = jnp.zeros_like(incoming[d])

        @pl.when(jnp.logical_not(exists[d]))
        def _():
            lent[d] = jnp.zeros_like(lent[d])

    def halo(d):
        return pltpu.make_async_remote_copy(
            src_ref=outgoing.at[d], dst_ref=incoming.at[d],
            send_sem=sent.at[0], recv_sem=halo_recv.at[d],
            device_id=target[d], device_id_type=MESH)

    def lend(d):
        return pltpu.make_async_remote_copy(
            src_ref=basis.at[:, pl.ds(own + d * BLK, BLK)], dst_ref=lent.at[d],
            send_sem=sent.at[0], recv_sem=lend_recv.at[d],
            device_id=target[opposite[d]], device_id_type=MESH)

    def lend_to(directions):
        for d in directions:
            @pl.when(exists[opposite[d]])
            def _():
                lend(d).start()

    def send(phase, src, dst, device):
        pltpu.make_async_remote_copy(
            src_ref=src, dst_ref=dst, send_sem=sent.at[0], recv_sem=bulk_recv.at[phase],
            device_id=device, device_id_type=MESH).start()

    def arrived(phase, buf, count):
        some = buf.at[pl.ds(0, count)]
        pltpu.make_async_copy(some, some, bulk_recv.at[phase]).wait()

    def drained(buf, count):
        some = buf.at[pl.ds(0, count)]
        pltpu.make_async_copy(some, some, sent.at[0]).wait()

    def spread_col(phase, buf, top, bot, ready, last=False):
        largest = jnp.maximum(jnp.abs(top), jnp.abs(bot))
        e, factor = scale_of(jnp.maximum(largest, half_roll(largest)))
        buf[c, :quarter] = to_words(top, bot, factor)
        buf[c, quarter:] = e[:1]
        ready()
        if not last:
            for offset in col_offsets:
                send(phase, buf.at[c], buf.at[c], (r, col_at(*offset)))
        for to in origin_first if last else ():
            @pl.when(c != to)
            def _():
                send(phase, buf.at[c], buf.at[c], (r, to))

    def gathered(buf):
        columns = []
        for first in range(0, ncol, 2):
            a, b = buf[first, :quarter], buf[first + 1, :quarter]
            words = jnp.where(low, a, half_roll(b)), jnp.where(low, half_roll(a), b)
            e = jnp.where(low1, buf[first, quarter:], buf[first + 1, quarter:])
            parts = [v for w in words for v in (w >> 24, (w << 16) >> 24)]
            parts += [v for w in words for v in ((w >> 16) & 0xFF, w & 0xFF)]
            parts.append(jnp.broadcast_to(e, (half, LANES)))
            columns.append(jnp.concatenate(parts, axis=0).astype(F32).astype(BF16))
        return jnp.concatenate(columns, axis=1)

    def select(codes, hot):
        part = matmul(codes, hot, NN)
        return (part[:rhs] * 256.0 + part[rhs:2 * rhs]).astype(jnp.int32), part[2 * rhs:2 * rhs + quarter].astype(jnp.int32)

    def halves(first, second):
        return jnp.where(low, first, half_roll(second)), jnp.where(low, half_roll(first), second)

    def largest_of(part):
        return functools.reduce(jnp.maximum, [jnp.abs(part[i:i + quarter]) for i in range(0, rhs, quarter)])

    def paired_words(part):
        e, factor = scale_of(largest_of(part))
        first = to_words(part[:quarter], part[quarter:half], factor)
        second = to_words(part[half:half + quarter], part[half + quarter:], factor)
        return list(zip(halves(first, second), (v[:1] for v in halves(e, e))))

    pl.semaphore_wait(barrier, nrow - 1 + len(greeted) + up.astype(jnp.int32) + down.astype(jnp.int32))
    for d in range(4):
        @pl.when(exists[d])
        def _():
            halo(d).start()

    for device in greeted:
        signal(passed.at[0], device)
    loads[0].wait()
    b_hi, b_lo = split(basis[...])
    basis2[:nev] = b_hi
    basis2[nev:] = b_lo
    partial = matmul(res_ref[...], basis2[:, :own], NT)

    pl.semaphore_wait(passed.at[0], len(greeted))
    for device in across_x:
        signal(passed.at[1], device)
    for d in range(4):
        @pl.when(exists[opposite[d]])
        def _():
            halo(d).wait_recv()

    inc = jnp.concatenate([incoming[d] for d in range(4)], axis=1)
    partial = partial + matmul(inc, basis2[:, own:], NT)
    partial = partial + half_roll(partial)
    spread_col(0, col1, jnp.where(low, partial[:quarter], partial[half:half + quarter]),
               jnp.where(low, partial[quarter:half], partial[half + quarter:]),
               lambda: pl.semaphore_wait(passed.at[1], NX - 1))

    span = rows // nz
    loads[1].wait()
    for t in range(nz):
        at = slice(t * span, (t + 1) * span)
        for h in range(2):
            turned = split(coarse[at, h * (width // 2):(h + 1) * (width // 2)].T)
            coarse_t[h * width:h * width + width // 2, at], coarse_t[h * width + width // 2:(h + 1) * width, at] = turned
    loads[2].wait()
    local = jnp.concatenate([res_ref[...], inc], axis=1)
    out_ref[...] = matmul(local, linv[...], NT)

    loads[5].wait()
    chunk = 2 * LANES
    place_in = lax.broadcasted_iota(jnp.int32, (width, chunk), 0) + c * width

    def build_in(i, carry):
        slot = slots_ref[:, pl.ds(pl.multiple_of(r * rows + i * chunk, chunk), chunk)]
        hot = jnp.where(place_in == slot, 1.0, 0.0).astype(BF16)
        hot_in[pl.ds(pl.multiple_of(i * chunk, chunk), chunk)] = hot.T
        return carry

    lax.fori_loop(0, rows // chunk, build_in, 0)

    arrived(0, col1, ncol - 1)
    partials = gathered(col1)
    part_blocks = width // 2 // LANES
    for h in range(2):
        codes, e = select(partials, hot_in[:, h * (width // 2):(h + 1) * (width // 2)])
        for q in range(part_blocks):
            at = slice(q * LANES, (q + 1) * LANES)
            row1[h, r, q * half:(q + 1) * half] = pack(codes[:half, at], codes[half:, at])
            row1[h, r, part_blocks * half + q:part_blocks * half + q + 1] = e[:1, at]
        for offset in row_offsets:
            send(1 + h, row1.at[h, r], row1.at[h, r], (row_at(*offset), c))

    lend_to((2, 3))

    def sides(at):
        return [((side, at, 0), (side, at, 1)) for side in (1, -1)]

    order = [((0, 0, 0), (0, 0, 1)), ((0, 1, 0), (0, 3, 1))] + sides(0)
    order += [((0, 1, 1), (0, 3, 0)), ((0, 2, 0), (0, 2, 1))] + sides(1) + sides(3) + sides(2)
    place = {key: 2 * i + j for i, pair in enumerate(order) for j, key in enumerate(pair)}
    wanted = []
    for keys in order:
        side = keys[0][0]
        safe = jnp.clip(c + side, 0, ncol - 1)
        pair = []
        for _, chip, k in keys:
            device = (chip * CORES + k) * ncol + safe
            at = pl.ds(pl.multiple_of((device // 2) * LANES, LANES), LANES)
            pair.append(jnp.broadcast_to(slots_ref[:, at], (8, LANES)))
        even = jnp.where(low, pair[0], half_roll(pair[1]))
        odd = jnp.where(low, half_roll(pair[0]), pair[1])
        both = jnp.where(lax.rem(safe, 2) == 0, even, odd)[:1]
        if side:
            both = jnp.where(exists[2] if side > 0 else exists[3], both, -1)
        wanted.append(both)
    wanted = jnp.concatenate(wanted, axis=1) - r * rows
    place_out = lax.broadcasted_iota(jnp.int32, (LANES, wanted.shape[1]), 0)

    def build_out(i, carry):
        hot = jnp.where(place_out == wanted - i * LANES, 1.0, 0.0)
        hot_out[pl.ds(pl.multiple_of(i * LANES, LANES), LANES)] = hot.astype(BF16)
        return carry

    lax.fori_loop(0, rows // LANES, build_out, 0)

    def column_half(h):
        arrived(1 + h, row1.at[h], nrow - 1)
        column = []
        for q in range(part_blocks):
            words = tree_sum([row1[h, i, q * half:(q + 1) * half] for i in range(nrow)])
            at = part_blocks * half + q
            scale = scale_from(tree_sum([row1[h, i, at:at + 1] for i in range(nrow)]))
            column.append(jnp.concatenate([v * scale for v in from_words(words)], axis=0))
        value = jnp.concatenate(split(jnp.concatenate(column, axis=1)), axis=0)
        return jnp.concatenate([value, value], axis=1)

    first_half = column_half(0)
    for t in range(nz):
        at = slice(t * span, (t + 1) * span)
        part = matmul(first_half, coarse_t[:width, at], NN)
        product[:, at] = part[:rhs] + part[rhs:]
    second_half = column_half(1)
    steps = far_first(nz) + [0]
    for batch in (steps[:2], steps[2:5], steps[5:]):
        parts = []
        for dz in batch:
            block = lax.rem(z + dz, nz)
            at = pl.ds(pl.multiple_of(block * span, span), span)
            part = matmul(second_half, coarse_t[width:, at], NN)
            parts.append((block, part[:rhs] + part[rhs:] + product[:, at]))
        for block, part in parts:
            for q in range(span // LANES):
                for i, (words, e) in enumerate(paired_words(part[:, q * LANES:(q + 1) * LANES])):
                    pieces[block * NX + 2 * q + i, :quarter] = words
                    pieces[block * NX + 2 * q + i, quarter:] = e
        for dz, (block, part) in zip(batch, parts):
            for dx in (2, 1, 3, 0) if dz else (2, 1, 3):
                to = block * NX + lax.rem(x + dx, NX)
                send(3, pieces.at[to], received.at[c], (r, to))

    lend_to((0, 1))
    received[c] = pieces[c]
    arrived(3, received, ncol - 1)
    tops, bots = [], []
    for i in range(ncol):
        scale = scale_from(received[i, quarter:])
        top, bot = from_words(received[i, :quarter])
        tops.append(top * scale)
        bots.append(bot * scale)
    top, bot = tree_sum(tops), tree_sum(bots)
    spread_col(4, col2, top, bot, lambda: None, True)

    wide[:nev] = basis2[:nev, :own]
    wide[6 * nev:7 * nev] = basis2[nev:, :own]
    for at in (5 * nev, 11 * nev):
        wide[at:at + nev] = jnp.zeros_like(wide[at:at + nev])
    for d in range(4):
        @pl.when(exists[d])
        def _():
            lend(d).wait_recv()

        l_hi, l_lo = split(lent[d])
        for b in range(own // BLK):
            here = ib_ref[0, d] == b
            at = slice(b * BLK, (b + 1) * BLK)
            wide[(d + 1) * nev:(d + 2) * nev, at] = jnp.where(here, l_hi, jnp.zeros_like(l_hi))
            wide[(d + 7) * nev:(d + 8) * nev, at] = jnp.where(here, l_lo, jnp.zeros_like(l_lo))

    arrived(4, col2, ncol - 1)
    solution = gathered(col2)
    groups = []
    for chips, stop in (((0,), 4), ((1, 3), 10), ((2,), 12)):
        start = len(groups) // 2
        codes, e = select(solution, hot_out[:, start * LANES:stop * LANES])
        for q in range(stop - start):
            at = slice(q * LANES, (q + 1) * LANES)
            words = halves(pack(codes[:quarter, at], codes[quarter:half, at]),
                           pack(codes[half:half + quarter, at], codes[half + quarter:, at]))
            groups.extend(zip(words, (v[:1] for v in halves(e[:, at], e[:, at]))))
        for chip in chips:
            for k in range(CORES):
                to = chip * CORES + k
                up_row = (0, *divmod((to + 1) % nrow, CORES))
                down_row = (0, *divmod((to - 1) % nrow, CORES))
                for i, key in enumerate(((0, chip, k), up_row, down_row, (1, chip, k), (-1, chip, k))):
                    words, e = groups[place[key]]
                    sets[to, i * quarter:(i + 1) * quarter] = words
                    sets[to, 5 * quarter + i:5 * quarter + i + 1] = e

                @pl.when(r != to)
                def _():
                    send(5, sets.at[to], row2.at[r], (to, c))
    row2[r] = sets[r]
    arrived(5, row2, nrow - 1)
    picks = []
    for k in range(5):
        words = tree_sum([row2[i, k * quarter:(k + 1) * quarter] for i in range(nrow)])
        at = 5 * quarter + k
        scale = scale_from(tree_sum([row2[i, at:at + 1] for i in range(nrow)]))
        picks.append([v * scale for v in from_words(words)])
    picks.append([jnp.zeros_like(picks[0][0])] * 2)
    columns = []
    for p in range(3):
        a, b = picks[2 * p], picks[2 * p + 1]
        columns.append(jnp.concatenate(
            [jnp.where(low, a[i], half_roll(b[i])) for i in range(2)]
            + [jnp.where(low, half_roll(a[i]), b[i]) for i in range(2)], axis=0))
    picked = jnp.concatenate(split(jnp.concatenate(columns, axis=1)), axis=0)
    inner = matmul(jnp.concatenate([picked, picked], axis=1), wide[...], NN)
    out_ref[...] = out_ref[...] + inner[:rhs] + inner[rhs:]

    drained(col1, ncol - 1)
    drained(row1.at[0], nrow - 1)
    drained(row1.at[1], nrow - 1)
    drained(received, ncol - 1)
    drained(col2, ncol - 1)
    drained(row2, nrow - 1)
    for d in range(4):
        @pl.when(exists[d])
        def _():
            halo(d).wait_send()

        @pl.when(exists[opposite[d]])
        def _():
            lend(d).wait_send()


def shards(nrow, ncol, residuals, intersect_blocks, local_inverse, coarse_basis, coarse_slots, coarse_inverse):
    own, rhs = residuals.shape
    loc, nev = coarse_basis.shape
    rows, width = coarse_inverse.shape
    total = coarse_slots.shape[0]
    assert 2 * nev == LANES and rows == ncol * nev and width == nrow * nev and loc == own + 4 * BLK and own % BLK == 0
    vmem = pl.BlockSpec(memory_space=pltpu.VMEM)
    hbm = pl.BlockSpec(memory_space=pl.ANY)
    dma = pltpu.SemaphoreType.DMA
    out = pl.pallas_call(
        functools.partial(kernel, nrow, ncol),
        name="schwarz",
        out_shape=pltpu.VMEM((rhs, own), F32),
        in_specs=[hbm] * 6,
        out_specs=vmem,
        scratch_shapes=[
            pltpu.VMEM((rhs, own), BF16),
            pltpu.SMEM(intersect_blocks.shape, jnp.int32),
            pltpu.VMEM((1, total), jnp.int32),
            pltpu.VMEM((4, rhs, BLK), BF16),
            pltpu.VMEM((4, rhs, BLK), BF16),
            pltpu.VMEM((own, loc), BF16),
            pltpu.VMEM((nev, loc), F32),
            pltpu.VMEM((2 * nev, loc), BF16),
            pltpu.VMEM((rows, width), F32),
            pltpu.VMEM((2 * width, rows), BF16),
            pltpu.VMEM((rows, width), BF16),
            pltpu.VMEM((rows, 3 * width), BF16),
            pltpu.VMEM((ncol, rhs // 4 + 1, LANES), jnp.int32),
            pltpu.VMEM((2, nrow, width // 2 // LANES * (rhs // 2 + 1), LANES), jnp.int32),
            pltpu.VMEM((rhs, rows), F32),
            pltpu.VMEM((ncol, rhs // 4 + 1, LANES), jnp.int32),
            pltpu.VMEM((ncol, rhs // 4 + 1, LANES), jnp.int32),
            pltpu.VMEM((ncol, rhs // 4 + 1, LANES), jnp.int32),
            pltpu.VMEM((nrow, 5 * (rhs // 4 + 1), LANES), jnp.int32),
            pltpu.VMEM((nrow, 5 * (rhs // 4 + 1), LANES), jnp.int32),
            pltpu.VMEM((4, nev, BLK), F32),
            pltpu.VMEM((12 * nev, own), BF16),
            dma((6,)),
            dma((1,)),
            dma((4,)),
            dma((4,)),
            dma((6,)),
            pltpu.SemaphoreType.REGULAR((2,)),
        ],
        compiler_params=pltpu.CompilerParams(collective_id=0, has_side_effects=True),
    )(
        residuals.T,
        intersect_blocks,
        local_inverse,
        coarse_basis.T,
        coarse_slots.reshape(1, total),
        coarse_inverse,
    )
    return out.T


def solution(mesh):
    placed = (
        P(("row", "col"), None),
        P(("row", "col"), None),
        P(("row", "col"), None),
        P(("row", "col"), None),
        P(),
        P("row", "col"),
    )
    return jax.shard_map(
        functools.partial(shards, mesh.shape["row"], mesh.shape["col"]),
        mesh=mesh, in_specs=placed, out_specs=P(("row", "col"), None), check_vma=False,
    )
```

```python
import functools

import jax
import jax.numpy as jnp
from jax import lax
from jax.experimental import pallas as pl
from jax.experimental.pallas import tpu as pltpu
from jax.sharding import PartitionSpec as P

MESH = pl.DeviceIdType.MESH
BLK = 128
LANES = 128
NX = 4
CORES = 2
PEAK = 32760.0
TINY = 1e-30
NT = (((1,), (1,)), ((), ()))
NN = (((1,), (0,)), ((), ()))
F32 = jnp.float32
BF16 = jnp.bfloat16


def matmul(a, b, dims):
    return lax.dot_general(a, b, dims, preferred_element_type=F32)


def split(x):
    hi = x.astype(BF16)
    return hi, (x - hi.astype(F32)).astype(BF16)


def lane_low(shape):
    return lax.broadcasted_iota(jnp.int32, shape, len(shape) - 1) < LANES // 2


def half_roll(x):
    return pltpu.roll(x, LANES // 2, 1)


def far_first(count):
    return sorted(range(1, count), key=lambda k: -min(k, count - k))


def tree_sum(parts):
    while len(parts) > 1:
        parts = [parts[i] + parts[i + 1] if i + 1 < len(parts) else parts[i] for i in range(0, len(parts), 2)]
    return parts[0]


def scale_of(largest):
    top = jnp.broadcast_to(jnp.max(largest, axis=0, keepdims=True), largest.shape)
    e = jnp.ceil(jnp.log2(jnp.maximum(top, TINY)))
    return e.astype(jnp.int32), jnp.exp2(-e) * PEAK


def scale_from(row):
    return jnp.exp2(row.astype(F32)) * (1.0 / PEAK)


def to_words(top, bot, factor):
    a = jnp.round(top * factor).astype(jnp.int32)
    b = jnp.round(bot * factor).astype(jnp.int32)
    return pack(a, b)


def pack(top, bot):
    return (top << 16) | (bot & 0xFFFF)


def from_words(w):
    return (w >> 16).astype(F32), ((w << 16) >> 16).astype(F32)


def kernel(
    nrow,
    ncol,
    res_hbm,
    ib_hbm,
    linv_hbm,
    basis_hbm,
    slots_hbm,
    coarse_hbm,
    out_ref,
    res_ref,
    ib_ref,
    slots_ref,
    outgoing,
    incoming,
    linv,
    basis,
    basis2,
    coarse,
    coarse_t,
    hot_in,
    hot_out,
    col1,
    row1,
    product,
    pieces,
    received,
    col2,
    sets,
    row2,
    lent,
    wide,
    load_sem,
    sent,
    halo_recv,
    lend_recv,
    bulk_recv,
    passed,
):
    r = lax.axis_index("row")
    c = lax.axis_index("col")
    z, x = c // NX, lax.rem(c, NX)
    y, core = r // CORES, lax.rem(r, CORES)
    nz, ny = ncol // NX, nrow // CORES
    rhs = res_ref.shape[0]
    own = res_ref.shape[1]
    half = rhs // 2
    quarter = rhs // 4
    rows, width = coarse.shape
    nev = basis.shape[0]
    low = lane_low((quarter, LANES))
    low1 = lane_low((1, LANES))

    col_offsets = sorted(
        ((dz, dx) for dz in range(nz) for dx in range(NX) if (dz, dx) != (0, 0)),
        key=lambda o: -(min(o[0], nz - o[0]) + min(o[1], NX - o[1])))
    row_offsets = sorted(
        ((dy, dk) for dy in range(ny) for dk in range(CORES) if (dy, dk) != (0, 0)),
        key=lambda o: -(min(o[0], ny - o[0]) + 0.5 * o[1]))

    rows_far_first = sorted(range(nrow), key=lambda i: (-min(i // CORES, ny - i // CORES), i % CORES))
    origin_first = sorted(range(ncol), key=lambda i: min(i // NX, nz - i // NX) + min(i % NX, NX - i % NX))

    def col_at(dz, dx):
        return lax.rem(z + dz, nz) * NX + lax.rem(x + dx, NX)

    def row_at(dy, dk):
        return lax.rem(y + dy, ny) * CORES + lax.rem(core + dk, CORES)

    exists = [r < nrow - 1, r > 0, c < ncol - 1, c > 0]
    target = [(r + 1, c), (r - 1, c), (r, c + 1), (r, c - 1)]
    opposite = [1, 0, 3, 2]

    loads = [
        pltpu.make_async_copy(basis_hbm, basis, load_sem.at[0]),
        pltpu.make_async_copy(coarse_hbm, coarse, load_sem.at[1]),
        pltpu.make_async_copy(linv_hbm, linv, load_sem.at[2]),
        pltpu.make_async_copy(res_hbm, res_ref, load_sem.at[3]),
        pltpu.make_async_copy(ib_hbm, ib_ref, load_sem.at[4]),
        pltpu.make_async_copy(slots_hbm, slots_ref, load_sem.at[5]),
    ]
    for i in (3, 4, 0):
        loads[i].start()

    def line_x(dx):
        return (r, z * NX + lax.rem(x + dx, NX))

    def line_z(dz):
        return (r, lax.rem(z + dz, nz) * NX + x)

    across_x = [line_x(dx) for dx in far_first(NX)]
    near_z = [line_z(dz) for dz in (2, nz - 2, 1, nz - 1)]
    greeted = across_x + near_z
    up = jnp.logical_and(x == NX - 1, exists[2])
    down = jnp.logical_and(x == 0, exists[3])
    barrier = pltpu.get_barrier_semaphore()

    def signal(sem, device):
        pl.semaphore_signal(sem, inc=1, device_id=device, device_id_type=MESH)

    @pl.when(up)
    def _():
        signal(barrier, target[2])

    @pl.when(down)
    def _():
        signal(barrier, target[3])

    for offset in row_offsets:
        signal(barrier, (row_at(*offset), c))
    for device in greeted:
        signal(barrier, device)
    for i in (5, 1, 2):
        loads[i].start()
    loads[4].wait()
    loads[3].wait()

    blocks = [res_ref[:, b * BLK:(b + 1) * BLK] for b in range(own // BLK)]
    for d in range(4):
        index = ib_ref[0, d]
        value = blocks[0]
        for b in range(1, len(blocks)):
            value = jnp.where(index == b, blocks[b], value)
        outgoing[d] = value

        @pl.when(jnp.logical_not(exists[opposite[d]]))
        def _():
            incoming[d] = jnp.zeros_like(incoming[d])

        @pl.when(jnp.logical_not(exists[d]))
        def _():
            lent[d] = jnp.zeros_like(lent[d])

    def halo(d):
        return pltpu.make_async_remote_copy(
            src_ref=outgoing.at[d], dst_ref=incoming.at[d],
            send_sem=sent.at[0], recv_sem=halo_recv.at[d],
            device_id=target[d], device_id_type=MESH)

    def lend(d):
        return pltpu.make_async_remote_copy(
            src_ref=basis.at[:, pl.ds(own + d * BLK, BLK)], dst_ref=lent.at[d],
            send_sem=sent.at[0], recv_sem=lend_recv.at[d],
            device_id=target[opposite[d]], device_id_type=MESH)

    def lend_to(directions):
        for d in directions:
            @pl.when(exists[opposite[d]])
            def _():
                lend(d).start()

    def send(phase, src, dst, device):
        pltpu.make_async_remote_copy(
            src_ref=src, dst_ref=dst, send_sem=sent.at[0], recv_sem=bulk_recv.at[phase],
            device_id=device, device_id_type=MESH).start()

    def arrived(phase, buf, count):
        some = buf.at[pl.ds(0, count)]
        pltpu.make_async_copy(some, some, bulk_recv.at[phase]).wait()

    def drained(buf, count):
        some = buf.at[pl.ds(0, count)]
        pltpu.make_async_copy(some, some, sent.at[0]).wait()

    def spread_col(phase, buf, top, bot, ready, last=False):
        largest = jnp.maximum(jnp.abs(top), jnp.abs(bot))
        e, factor = scale_of(jnp.maximum(largest, half_roll(largest)))
        buf[c, :quarter] = to_words(top, bot, factor)
        buf[c, quarter:] = e[:1]
        ready()
        if not last:
            for offset in col_offsets:
                send(phase, buf.at[c], buf.at[c], (r, col_at(*offset)))
        for to in origin_first if last else ():
            @pl.when(c != to)
            def _():
                send(phase, buf.at[c], buf.at[c], (r, to))

    def gathered(buf):
        columns = []
        for first in range(0, ncol, 2):
            a, b = buf[first, :quarter], buf[first + 1, :quarter]
            words = jnp.where(low, a, half_roll(b)), jnp.where(low, half_roll(a), b)
            e = jnp.where(low1, buf[first, quarter:], buf[first + 1, quarter:])
            parts = [v for w in words for v in (w >> 24, (w << 16) >> 24)]
            parts += [v for w in words for v in ((w >> 16) & 0xFF, w & 0xFF)]
            parts.append(jnp.broadcast_to(e, (half, LANES)))
            columns.append(jnp.concatenate(parts, axis=0).astype(F32).astype(BF16))
        return jnp.concatenate(columns, axis=1)

    def select(codes, hot):
        part = matmul(codes, hot, NN)
        return (part[:rhs] * 256.0 + part[rhs:2 * rhs]).astype(jnp.int32), part[2 * rhs:2 * rhs + quarter].astype(jnp.int32)

    def halves(first, second):
        return jnp.where(low, first, half_roll(second)), jnp.where(low, half_roll(first), second)

    def largest_of(part):
        return functools.reduce(jnp.maximum, [jnp.abs(part[i:i + quarter]) for i in range(0, rhs, quarter)])

    def paired_words(part):
        e, factor = scale_of(largest_of(part))
        first = to_words(part[:quarter], part[quarter:half], factor)
        second = to_words(part[half:half + quarter], part[half + quarter:], factor)
        return list(zip(halves(first, second), (v[:1] for v in halves(e, e))))

    pl.semaphore_wait(barrier, nrow - 1 + len(greeted) + up.astype(jnp.int32) + down.astype(jnp.int32))
    for d in range(4):
        @pl.when(exists[d])
        def _():
            halo(d).start()

    for device in greeted:
        signal(passed.at[0], device)
    loads[0].wait()
    b_hi, b_lo = split(basis[...])
    basis2[:nev] = b_hi
    basis2[nev:] = b_lo
    partial = matmul(res_ref[...], basis2[:, :own], NT)

    pl.semaphore_wait(passed.at[0], len(greeted))
    for device in across_x:
        signal(passed.at[1], device)
    for d in range(4):
        @pl.when(exists[opposite[d]])
        def _():
            halo(d).wait_recv()

    inc = jnp.concatenate([incoming[d] for d in range(4)], axis=1)
    partial = partial + matmul(inc, basis2[:, own:], NT)
    partial = partial + half_roll(partial)
    spread_col(0, col1, jnp.where(low, partial[:quarter], partial[half:half + quarter]),
               jnp.where(low, partial[quarter:half], partial[half + quarter:]),
               lambda: pl.semaphore_wait(passed.at[1], NX - 1))

    span = rows // nz
    loads[1].wait()
    for t in range(nz):
        at = slice(t * span, (t + 1) * span)
        for h in range(2):
            turned = split(coarse[at, h * (width // 2):(h + 1) * (width // 2)].T)
            coarse_t[h * width:h * width + width // 2, at], coarse_t[h * width + width // 2:(h + 1) * width, at] = turned
    loads[2].wait()
    local = jnp.concatenate([res_ref[...], inc], axis=1)
    out_ref[...] = matmul(local, linv[...], NT)

    loads[5].wait()
    chunk = 2 * LANES
    place_in = lax.broadcasted_iota(jnp.int32, (width, chunk), 0) + c * width

    def build_in(i, carry):
        slot = slots_ref[:, pl.ds(pl.multiple_of(r * rows + i * chunk, chunk), chunk)]
        hot = jnp.where(place_in == slot, 1.0, 0.0).astype(BF16)
        hot_in[pl.ds(pl.multiple_of(i * chunk, chunk), chunk)] = hot.T
        return carry

    lax.fori_loop(0, rows // chunk, build_in, 0)

    arrived(0, col1, ncol - 1)
    partials = gathered(col1)
    part_blocks = width // 2 // LANES
    for h in range(2):
        codes, e = select(partials, hot_in[:, h * (width // 2):(h + 1) * (width // 2)])
        for q in range(part_blocks):
            at = slice(q * LANES, (q + 1) * LANES)
            row1[h, r, q * half:(q + 1) * half] = pack(codes[:half, at], codes[half:, at])
            row1[h, r, part_blocks * half + q:part_blocks * half + q + 1] = e[:1, at]
        for to in rows_far_first:
            @pl.when(r != to)
            def _():
                send(1 + h, row1.at[h, r], row1.at[h, r], (to, c))


    lend_to((2, 3))

    def sides(at):
        return [((side, at, 0), (side, at, 1)) for side in (1, -1)]

    order = [((0, 0, 0), (0, 0, 1)), ((0, 1, 0), (0, 3, 1))] + sides(0)
    order += [((0, 1, 1), (0, 3, 0)), ((0, 2, 0), (0, 2, 1))] + sides(1) + sides(3) + sides(2)
    place = {key: 2 * i + j for i, pair in enumerate(order) for j, key in enumerate(pair)}
    wanted = []
    for keys in order:
        side = keys[0][0]
        safe = jnp.clip(c + side, 0, ncol - 1)
        pair = []
        for _, chip, k in keys:
            device = (chip * CORES + k) * ncol + safe
            at = pl.ds(pl.multiple_of((device // 2) * LANES, LANES), LANES)
            pair.append(jnp.broadcast_to(slots_ref[:, at], (8, LANES)))
        even = jnp.where(low, pair[0], half_roll(pair[1]))
        odd = jnp.where(low, half_roll(pair[0]), pair[1])
        both = jnp.where(lax.rem(safe, 2) == 0, even, odd)[:1]
        if side:
            both = jnp.where(exists[2] if side > 0 else exists[3], both, -1)
        wanted.append(both)
    wanted = jnp.concatenate(wanted, axis=1) - r * rows
    place_out = lax.broadcasted_iota(jnp.int32, (LANES, wanted.shape[1]), 0)

    def build_out(i, carry):
        hot = jnp.where(place_out == wanted - i * LANES, 1.0, 0.0)
        hot_out[pl.ds(pl.multiple_of(i * LANES, LANES), LANES)] = hot.astype(BF16)
        return carry

    lax.fori_loop(0, rows // LANES, build_out, 0)

    def column_half(h):
        arrived(1 + h, row1.at[h], nrow - 1)
        column = []
        for q in range(part_blocks):
            words = tree_sum([row1[h, i, q * half:(q + 1) * half] for i in range(nrow)])
            at = part_blocks * half + q
            scale = scale_from(tree_sum([row1[h, i, at:at + 1] for i in range(nrow)]))
            column.append(jnp.concatenate([v * scale for v in from_words(words)], axis=0))
        value = jnp.concatenate(split(jnp.concatenate(column, axis=1)), axis=0)
        return jnp.concatenate([value, value], axis=1)

    first_half = column_half(0)
    for t in range(nz):
        at = slice(t * span, (t + 1) * span)
        part = matmul(first_half, coarse_t[:width, at], NN)
        product[:, at] = part[:rhs] + part[rhs:]
    second_half = column_half(1)
    steps = far_first(nz) + [0]
    for batch in (steps[:2], steps[2:5], steps[5:]):
        parts = []
        for dz in batch:
            block = lax.rem(z + dz, nz)
            at = pl.ds(pl.multiple_of(block * span, span), span)
            part = matmul(second_half, coarse_t[width:, at], NN)
            parts.append((block, part[:rhs] + part[rhs:] + product[:, at]))
        for block, part in parts:
            for q in range(span // LANES):
                for i, (words, e) in enumerate(paired_words(part[:, q * LANES:(q + 1) * LANES])):
                    pieces[block * NX + 2 * q + i, :quarter] = words
                    pieces[block * NX + 2 * q + i, quarter:] = e
        for dz, (block, part) in zip(batch, parts):
            for dx in (2, 1, 3, 0) if dz else (2, 1, 3):
                to = block * NX + lax.rem(x + dx, NX)
                send(3, pieces.at[to], received.at[c], (r, to))

    lend_to((0, 1))
    received[c] = pieces[c]
    arrived(3, received, ncol - 1)
    tops, bots = [], []
    for i in range(ncol):
        scale = scale_from(received[i, quarter:])
        top, bot = from_words(received[i, :quarter])
        tops.append(top * scale)
        bots.append(bot * scale)
    top, bot = tree_sum(tops), tree_sum(bots)
    spread_col(4, col2, top, bot, lambda: None, True)

    wide[:nev] = basis2[:nev, :own]
    wide[6 * nev:7 * nev] = basis2[nev:, :own]
    for at in (5 * nev, 11 * nev):
        wide[at:at + nev] = jnp.zeros_like(wide[at:at + nev])
    for d in range(4):
        @pl.when(exists[d])
        def _():
            lend(d).wait_recv()

        l_hi, l_lo = split(lent[d])
        for b in range(own // BLK):
            here = ib_ref[0, d] == b
            at = slice(b * BLK, (b + 1) * BLK)
            wide[(d + 1) * nev:(d + 2) * nev, at] = jnp.where(here, l_hi, jnp.zeros_like(l_hi))
            wide[(d + 7) * nev:(d + 8) * nev, at] = jnp.where(here, l_lo, jnp.zeros_like(l_lo))

    arrived(4, col2, ncol - 1)
    solution = gathered(col2)
    groups = []
    for chips, stop in (((0,), 4), ((1, 3), 10), ((2,), 12)):
        start = len(groups) // 2
        codes, e = select(solution, hot_out[:, start * LANES:stop * LANES])
        for q in range(stop - start):
            at = slice(q * LANES, (q + 1) * LANES)
            words = halves(pack(codes[:quarter, at], codes[quarter:half, at]),
                           pack(codes[half:half + quarter, at], codes[half + quarter:, at]))
            groups.extend(zip(words, (v[:1] for v in halves(e[:, at], e[:, at]))))
        for chip in chips:
            for k in reversed(range(CORES)):
                to = chip * CORES + k
                up_row = (0, *divmod((to + 1) % nrow, CORES))
                down_row = (0, *divmod((to - 1) % nrow, CORES))
                for i, key in enumerate(((0, chip, k), up_row, down_row, (1, chip, k), (-1, chip, k))):
                    words, e = groups[place[key]]
                    sets[to, i * quarter:(i + 1) * quarter] = words
                    sets[to, 5 * quarter + i:5 * quarter + i + 1] = e

                @pl.when(r != to)
                def _():
                    send(5, sets.at[to], row2.at[r], (to, c))
    row2[r] = sets[r]
    arrived(5, row2, nrow - 1)
    picks = []
    for k in range(5):
        words = tree_sum([row2[i, k * quarter:(k + 1) * quarter] for i in range(nrow)])
        at = 5 * quarter + k
        scale = scale_from(tree_sum([row2[i, at:at + 1] for i in range(nrow)]))
        picks.append([v * scale for v in from_words(words)])
    picks.append([jnp.zeros_like(picks[0][0])] * 2)
    columns = []
    for p in range(3):
        a, b = picks[2 * p], picks[2 * p + 1]
        columns.append(jnp.concatenate(
            [jnp.where(low, a[i], half_roll(b[i])) for i in range(2)]
            + [jnp.where(low, half_roll(a[i]), b[i]) for i in range(2)], axis=0))
    picked = jnp.concatenate(split(jnp.concatenate(columns, axis=1)), axis=0)
    inner = matmul(jnp.concatenate([picked, picked], axis=1), wide[...], NN)
    out_ref[...] = out_ref[...] + inner[:rhs] + inner[rhs:]

    drained(col1, ncol - 1)
    drained(row1.at[0], nrow - 1)
    drained(row1.at[1], nrow - 1)
    drained(received, ncol - 1)
    drained(col2, ncol - 1)
    drained(row2, nrow - 1)
    for d in range(4):
        @pl.when(exists[d])
        def _():
            halo(d).wait_send()

        @pl.when(exists[opposite[d]])
        def _():
            lend(d).wait_send()


def shards(nrow, ncol, residuals, intersect_blocks, local_inverse, coarse_basis, coarse_slots, coarse_inverse):
    own, rhs = residuals.shape
    loc, nev = coarse_basis.shape
    rows, width = coarse_inverse.shape
    total = coarse_slots.shape[0]
    assert 2 * nev == LANES and rows == ncol * nev and width == nrow * nev and loc == own + 4 * BLK and own % BLK == 0
    vmem = pl.BlockSpec(memory_space=pltpu.VMEM)
    hbm = pl.BlockSpec(memory_space=pl.ANY)
    dma = pltpu.SemaphoreType.DMA
    out = pl.pallas_call(
        functools.partial(kernel, nrow, ncol),
        name="schwarz",
        out_shape=pltpu.VMEM((rhs, own), F32),
        in_specs=[hbm] * 6,
        out_specs=vmem,
        scratch_shapes=[
            pltpu.VMEM((rhs, own), BF16),
            pltpu.SMEM(intersect_blocks.shape, jnp.int32),
            pltpu.VMEM((1, total), jnp.int32),
            pltpu.VMEM((4, rhs, BLK), BF16),
            pltpu.VMEM((4, rhs, BLK), BF16),
            pltpu.VMEM((own, loc), BF16),
            pltpu.VMEM((nev, loc), F32),
            pltpu.VMEM((2 * nev, loc), BF16),
            pltpu.VMEM((rows, width), F32),
            pltpu.VMEM((2 * width, rows), BF16),
            pltpu.VMEM((rows, width), BF16),
            pltpu.VMEM((rows, 3 * width), BF16),
            pltpu.VMEM((ncol, rhs // 4 + 1, LANES), jnp.int32),
            pltpu.VMEM((2, nrow, width // 2 // LANES * (rhs // 2 + 1), LANES), jnp.int32),
            pltpu.VMEM((rhs, rows), F32),
            pltpu.VMEM((ncol, rhs // 4 + 1, LANES), jnp.int32),
            pltpu.VMEM((ncol, rhs // 4 + 1, LANES), jnp.int32),
            pltpu.VMEM((ncol, rhs // 4 + 1, LANES), jnp.int32),
            pltpu.VMEM((nrow, 5 * (rhs // 4 + 1), LANES), jnp.int32),
            pltpu.VMEM((nrow, 5 * (rhs // 4 + 1), LANES), jnp.int32),
            pltpu.VMEM((4, nev, BLK), F32),
            pltpu.VMEM((12 * nev, own), BF16),
            dma((6,)),
            dma((1,)),
            dma((4,)),
            dma((4,)),
            dma((6,)),
            pltpu.SemaphoreType.REGULAR((2,)),
        ],
        compiler_params=pltpu.CompilerParams(collective_id=0, has_side_effects=True),
    )(
        residuals.T,
        intersect_blocks,
        local_inverse,
        coarse_basis.T,
        coarse_slots.reshape(1, total),
        coarse_inverse,
    )
    return out.T


def solution(mesh):
    placed = (
        P(("row", "col"), None),
        P(("row", "col"), None),
        P(("row", "col"), None),
        P(("row", "col"), None),
        P(),
        P("row", "col"),
    )
    return jax.shard_map(
        functools.partial(shards, mesh.shape["row"], mesh.shape["col"]),
        mesh=mesh, in_specs=placed, out_specs=P(("row", "col"), None), check_vma=False,
    )
```

```python
import functools

import jax
import jax.numpy as jnp
from jax import lax
from jax.experimental import pallas as pl
from jax.experimental.pallas import tpu as pltpu
from jax.sharding import PartitionSpec as P

MESH = pl.DeviceIdType.MESH
BLK = 128
LANES = 128
NX = 4
CORES = 2
PEAK = 32760.0
TINY = 1e-33
NT = (((1,), (1,)), ((), ()))
NN = (((1,), (0,)), ((), ()))
F32 = jnp.float32
BF16 = jnp.bfloat16


def matmul(a, b, dims):
    return lax.dot_general(a, b, dims, preferred_element_type=F32)


def split(x):
    hi = x.astype(BF16)
    return hi, (x - hi.astype(F32)).astype(BF16)


def lane_low(shape):
    return lax.broadcasted_iota(jnp.int32, shape, len(shape) - 1) < LANES // 2


def half_roll(x):
    return pltpu.roll(x, LANES // 2, 1)


def far_first(count):
    return sorted(range(1, count), key=lambda k: -min(k, count - k))


def tree_sum(parts):
    while len(parts) > 1:
        parts = [parts[i] + parts[i + 1] if i + 1 < len(parts) else parts[i] for i in range(0, len(parts), 2)]
    return parts[0]


def scale_of(largest):
    top = jnp.broadcast_to(jnp.max(largest, axis=0, keepdims=True), largest.shape)
    e = jnp.ceil(jnp.log2(jnp.maximum(top, TINY)))
    return e.astype(jnp.int32), jnp.exp2(-e) * PEAK


def scale_from(row):
    return jnp.exp2(row.astype(F32)) * (1.0 / PEAK)


def to_words(top, bot, factor):
    a = jnp.round(top * factor).astype(jnp.int32)
    b = jnp.round(bot * factor).astype(jnp.int32)
    return pack(a, b)


def pack(top, bot):
    return (top << 16) | (bot & 0xFFFF)


def from_words(w):
    return (w >> 16).astype(F32), ((w << 16) >> 16).astype(F32)


def kernel(
    nrow,
    ncol,
    res_hbm,
    ib_hbm,
    linv_hbm,
    basis_hbm,
    slots_hbm,
    coarse_hbm,
    out_ref,
    res_ref,
    ib_ref,
    slots_ref,
    outgoing,
    incoming,
    linv,
    basis,
    basis2,
    basis_t,
    coarse,
    coarse_t,
    hot_in,
    hot_out,
    col1,
    row1,
    product,
    pieces,
    received,
    col2,
    sets,
    row2,
    lent,
    wide,
    load_sem,
    sent,
    halo_recv,
    lend_recv,
    bulk_recv,
    passed,
):
    r = lax.axis_index("row")
    c = lax.axis_index("col")
    z, x = c // NX, lax.rem(c, NX)
    y, core = r // CORES, lax.rem(r, CORES)
    nz, ny = ncol // NX, nrow // CORES
    rhs = res_ref.shape[0]
    own = res_ref.shape[1]
    half = rhs // 2
    quarter = rhs // 4
    rows, width = coarse.shape
    nev = basis.shape[0]
    low = lane_low((quarter, LANES))
    low1 = lane_low((1, LANES))

    col_offsets = sorted(
        ((dz, dx) for dz in range(nz) for dx in range(NX) if (dz, dx) != (0, 0)),
        key=lambda o: -(min(o[0], nz - o[0]) + min(o[1], NX - o[1])))
    row_offsets = sorted(
        ((dy, dk) for dy in range(ny) for dk in range(CORES) if (dy, dk) != (0, 0)),
        key=lambda o: -(min(o[0], ny - o[0]) + 0.5 * o[1]))

    rows_far_first = sorted(range(nrow), key=lambda i: (-min(i // CORES, ny - i // CORES), i % CORES))

    def col_at(dz, dx):
        return lax.rem(z + dz, nz) * NX + lax.rem(x + dx, NX)

    def row_at(dy, dk):
        return lax.rem(y + dy, ny) * CORES + lax.rem(core + dk, CORES)

    exists = [r < nrow - 1, r > 0, c < ncol - 1, c > 0]
    target = [(r + 1, c), (r - 1, c), (r, c + 1), (r, c - 1)]
    opposite = [1, 0, 3, 2]

    loads = [
        pltpu.make_async_copy(basis_hbm, basis, load_sem.at[0]),
        pltpu.make_async_copy(coarse_hbm, coarse, load_sem.at[1]),
        pltpu.make_async_copy(linv_hbm, linv, load_sem.at[2]),
        pltpu.make_async_copy(res_hbm, res_ref, load_sem.at[3]),
        pltpu.make_async_copy(ib_hbm, ib_ref, load_sem.at[4]),
        pltpu.make_async_copy(slots_hbm, slots_ref, load_sem.at[5]),
    ]
    for i in (3, 4, 0):
        loads[i].start()

    def line_x(dx):
        return (r, z * NX + lax.rem(x + dx, NX))

    def line_z(dz):
        return (r, lax.rem(z + dz, nz) * NX + x)

    across_x = [line_x(dx) for dx in far_first(NX)]
    near_z = [line_z(dz) for dz in (2, nz - 2, 1, nz - 1)]
    greeted = across_x + near_z
    up = jnp.logical_and(x == NX - 1, exists[2])
    down = jnp.logical_and(x == 0, exists[3])
    barrier = pltpu.get_barrier_semaphore()

    def signal(sem, device):
        pl.semaphore_signal(sem, inc=1, device_id=device, device_id_type=MESH)

    @pl.when(up)
    def _():
        signal(barrier, target[2])

    @pl.when(down)
    def _():
        signal(barrier, target[3])

    for offset in row_offsets:
        signal(barrier, (row_at(*offset), c))
    for device in greeted:
        signal(barrier, device)
    for i in (5, 1, 2):
        loads[i].start()
    loads[4].wait()
    loads[3].wait()

    blocks = [res_ref[:, b * BLK:(b + 1) * BLK] for b in range(own // BLK)]
    for d in range(4):
        index = ib_ref[0, d]
        value = blocks[0]
        for b in range(1, len(blocks)):
            value = jnp.where(index == b, blocks[b], value)
        outgoing[d] = value

        @pl.when(jnp.logical_not(exists[opposite[d]]))
        def _():
            incoming[d] = jnp.zeros_like(incoming[d])

        @pl.when(jnp.logical_not(exists[d]))
        def _():
            lent[d] = jnp.zeros_like(lent[d])

    def halo(d):
        return pltpu.make_async_remote_copy(
            src_ref=outgoing.at[d], dst_ref=incoming.at[d],
            send_sem=sent.at[0], recv_sem=halo_recv.at[d],
            device_id=target[d], device_id_type=MESH)

    def lend(d):
        return pltpu.make_async_remote_copy(
            src_ref=basis.at[:, pl.ds(own + d * BLK, BLK)], dst_ref=lent.at[d],
            send_sem=sent.at[0], recv_sem=lend_recv.at[d],
            device_id=target[opposite[d]], device_id_type=MESH)

    def lend_to(directions):
        for d in directions:
            @pl.when(exists[opposite[d]])
            def _():
                lend(d).start()

    def send(phase, src, dst, device):
        pltpu.make_async_remote_copy(
            src_ref=src, dst_ref=dst, send_sem=sent.at[0], recv_sem=bulk_recv.at[phase],
            device_id=device, device_id_type=MESH).start()

    def arrived(phase, buf, count):
        some = buf.at[pl.ds(0, count)]
        pltpu.make_async_copy(some, some, bulk_recv.at[phase]).wait()

    def drained(buf, count):
        some = buf.at[pl.ds(0, count)]
        pltpu.make_async_copy(some, some, sent.at[0]).wait()

    def spread_col(phase, buf, top, bot, ready, last=False):
        largest = jnp.maximum(jnp.abs(top), jnp.abs(bot))
        e, factor = scale_of(jnp.maximum(largest, half_roll(largest)))
        buf[c, :quarter] = to_words(top, bot, factor)
        buf[c, quarter:] = e[:1]
        ready()
        if not last:
            for offset in col_offsets:
                send(phase, buf.at[c], buf.at[c], (r, col_at(*offset)))
        if last:
            @pl.when(c != 0)
            def _():
                send(phase, buf.at[c], buf.at[c], (r, 0))

            for offset in col_offsets:
                to = col_at(*offset)

                @pl.when(to != 0)
                def _():
                    send(phase, buf.at[c], buf.at[c], (r, to))

    def gathered(buf):
        columns = []
        for first in range(0, ncol, 2):
            a, b = buf[first, :quarter], buf[first + 1, :quarter]
            words = jnp.where(low, a, half_roll(b)), jnp.where(low, half_roll(a), b)
            e = jnp.where(low1, buf[first, quarter:], buf[first + 1, quarter:])
            parts = [v for w in words for v in (w >> 24, (w << 16) >> 24)]
            parts += [v for w in words for v in ((w >> 16) & 0xFF, w & 0xFF)]
            parts.append(jnp.broadcast_to(e, (half, LANES)))
            columns.append(jnp.concatenate(parts, axis=0).astype(F32).astype(BF16))
        return jnp.concatenate(columns, axis=1)

    def select(codes, hot):
        part = matmul(codes, hot, NN)
        return (part[:rhs] * 256.0 + part[rhs:2 * rhs]).astype(jnp.int32), part[2 * rhs:2 * rhs + quarter].astype(jnp.int32)

    def halves(first, second):
        return jnp.where(low, first, half_roll(second)), jnp.where(low, half_roll(first), second)

    def largest_of(part):
        return functools.reduce(jnp.maximum, [jnp.abs(part[i:i + quarter]) for i in range(0, rhs, quarter)])

    def paired_words(part):
        e, factor = scale_of(largest_of(part))
        first = to_words(part[:quarter], part[quarter:half], factor)
        second = to_words(part[half:half + quarter], part[half + quarter:], factor)
        return list(zip(halves(first, second), (v[:1] for v in halves(e, e))))

    pl.semaphore_wait(barrier, nrow - 1 + len(greeted) + up.astype(jnp.int32) + down.astype(jnp.int32))
    for d in range(4):
        @pl.when(exists[d])
        def _():
            halo(d).start()

    for device in greeted:
        signal(passed.at[0], device)
    loads[0].wait()
    b_hi, b_lo = split(basis[...])
    basis2[:nev] = b_hi
    basis2[nev:] = b_lo
    partial = matmul(res_ref[...], basis2[:, :own], NT)
    basis_t[...] = basis2[:, own:].T

    pl.semaphore_wait(passed.at[0], len(greeted))
    for device in across_x:
        signal(passed.at[1], device)
    for d in range(4):
        @pl.when(exists[opposite[d]])
        def _():
            halo(d).wait_recv()

    inc = jnp.concatenate([incoming[d] for d in range(4)], axis=1)
    partial = partial + matmul(inc, basis_t[...], NN)
    partial = partial + half_roll(partial)
    spread_col(0, col1, jnp.where(low, partial[:quarter], partial[half:half + quarter]),
               jnp.where(low, partial[quarter:half], partial[half + quarter:]),
               lambda: pl.semaphore_wait(passed.at[1], NX - 1))

    span = rows // nz
    loads[1].wait()
    for t in range(nz):
        at = slice(t * span, (t + 1) * span)
        for h in range(2):
            turned = split(coarse[at, h * (width // 2):(h + 1) * (width // 2)].T)
            coarse_t[h * width:h * width + width // 2, at], coarse_t[h * width + width // 2:(h + 1) * width, at] = turned
    loads[2].wait()
    local = jnp.concatenate([res_ref[...], inc], axis=1)
    out_ref[...] = matmul(local, linv[...], NT)

    loads[5].wait()
    chunk = 2 * LANES
    place_in = lax.broadcasted_iota(jnp.int32, (width, chunk), 0) + c * width

    def build_in(i, carry):
        slot = slots_ref[:, pl.ds(pl.multiple_of(r * rows + i * chunk, chunk), chunk)]
        hot = jnp.where(place_in == slot, 1.0, 0.0).astype(BF16)
        hot_in[pl.ds(pl.multiple_of(i * chunk, chunk), chunk)] = hot.T
        return carry

    lax.fori_loop(0, rows // chunk, build_in, 0)

    arrived(0, col1, ncol - 1)
    partials = gathered(col1)
    part_blocks = width // 2 // LANES
    for h in range(2):
        codes, e = select(partials, hot_in[:, h * (width // 2):(h + 1) * (width // 2)])
        for q in range(part_blocks):
            at = slice(q * LANES, (q + 1) * LANES)
            row1[h, r, q * half:(q + 1) * half] = pack(codes[:half, at], codes[half:, at])
            row1[h, r, part_blocks * half + q:part_blocks * half + q + 1] = e[:1, at]
        for to in rows_far_first:
            @pl.when(r != to)
            def _():
                send(1 + h, row1.at[h, r], row1.at[h, r], (to, c))


    lend_to((2, 3))

    def sides(at):
        return [((side, at, 0), (side, at, 1)) for side in (1, -1)]

    order = [((0, 0, 0), (0, 0, 1)), ((0, 1, 0), (0, 3, 1))] + sides(0)
    order += [((0, 1, 1), (0, 3, 0)), ((0, 2, 0), (0, 2, 1))] + sides(1) + sides(3) + sides(2)
    place = {key: 2 * i + j for i, pair in enumerate(order) for j, key in enumerate(pair)}
    wanted = []
    for keys in order:
        side = keys[0][0]
        safe = jnp.clip(c + side, 0, ncol - 1)
        pair = []
        for _, chip, k in keys:
            device = (chip * CORES + k) * ncol + safe
            at = pl.ds(pl.multiple_of((device // 2) * LANES, LANES), LANES)
            pair.append(jnp.broadcast_to(slots_ref[:, at], (8, LANES)))
        even = jnp.where(low, pair[0], half_roll(pair[1]))
        odd = jnp.where(low, half_roll(pair[0]), pair[1])
        both = jnp.where(lax.rem(safe, 2) == 0, even, odd)[:1]
        if side:
            both = jnp.where(exists[2] if side > 0 else exists[3], both, -1)
        wanted.append(both)
    wanted = jnp.concatenate(wanted, axis=1) - r * rows
    place_out = lax.broadcasted_iota(jnp.int32, (LANES, wanted.shape[1]), 0)

    def build_out(i, carry):
        hot = jnp.where(place_out == wanted - i * LANES, 1.0, 0.0)
        hot_out[pl.ds(pl.multiple_of(i * LANES, LANES), LANES)] = hot.astype(BF16)
        return carry

    lax.fori_loop(0, rows // LANES, build_out, 0)

    def column_half(h):
        arrived(1 + h, row1.at[h], nrow - 1)
        column = []
        for q in range(part_blocks):
            words = tree_sum([row1[h, i, q * half:(q + 1) * half] for i in range(nrow)])
            at = part_blocks * half + q
            scale = scale_from(tree_sum([row1[h, i, at:at + 1] for i in range(nrow)]))
            column.append(jnp.concatenate([v * scale for v in from_words(words)], axis=0))
        value = jnp.concatenate(split(jnp.concatenate(column, axis=1)), axis=0)
        return jnp.concatenate([value, value], axis=1)

    first_half = column_half(0)
    for t in range(nz):
        at = slice(t * span, (t + 1) * span)
        part = matmul(first_half, coarse_t[:width, at], NN)
        product[:, at] = part[:rhs] + part[rhs:]
    second_half = column_half(1)
    steps = far_first(nz) + [0]
    for batch in (steps[:2], steps[2:5], steps[5:]):
        parts = []
        for dz in batch:
            block = lax.rem(z + dz, nz)
            at = pl.ds(pl.multiple_of(block * span, span), span)
            part = matmul(second_half, coarse_t[width:, at], NN)
            parts.append((block, part[:rhs] + part[rhs:] + product[:, at]))
        for block, part in parts:
            for q in range(span // LANES):
                for i, (words, e) in enumerate(paired_words(part[:, q * LANES:(q + 1) * LANES])):
                    pieces[block * NX + 2 * q + i, :quarter] = words
                    pieces[block * NX + 2 * q + i, quarter:] = e
        for dz, (block, part) in zip(batch, parts):
            for dx in (2, 1, 3, 0) if dz else (2, 1, 3):
                to = block * NX + lax.rem(x + dx, NX)
                send(3, pieces.at[to], received.at[c], (r, to))

    lend_to((0, 1))
    received[c] = pieces[c]
    arrived(3, received, ncol - 1)
    tops, bots = [], []
    for i in range(ncol):
        scale = scale_from(received[i, quarter:])
        top, bot = from_words(received[i, :quarter])
        tops.append(top * scale)
        bots.append(bot * scale)
    top, bot = tree_sum(tops), tree_sum(bots)
    spread_col(4, col2, top, bot, lambda: None, True)

    wide[:nev] = basis2[:nev, :own]
    wide[6 * nev:7 * nev] = basis2[nev:, :own]
    for at in (5 * nev, 11 * nev):
        wide[at:at + nev] = jnp.zeros_like(wide[at:at + nev])
    for d in range(4):
        @pl.when(exists[d])
        def _():
            lend(d).wait_recv()

        l_hi, l_lo = split(lent[d])
        for b in range(own // BLK):
            here = ib_ref[0, d] == b
            at = slice(b * BLK, (b + 1) * BLK)
            wide[(d + 1) * nev:(d + 2) * nev, at] = jnp.where(here, l_hi, jnp.zeros_like(l_hi))
            wide[(d + 7) * nev:(d + 8) * nev, at] = jnp.where(here, l_lo, jnp.zeros_like(l_lo))

    arrived(4, col2, ncol - 1)
    solution = gathered(col2)
    groups = []
    for chips, stop in (((0,), 4), ((1, 3), 10), ((2,), 12)):
        start = len(groups) // 2
        codes, e = select(solution, hot_out[:, start * LANES:stop * LANES])
        for q in range(stop - start):
            at = slice(q * LANES, (q + 1) * LANES)
            words = halves(pack(codes[:quarter, at], codes[quarter:half, at]),
                           pack(codes[half:half + quarter, at], codes[half + quarter:, at]))
            groups.extend(zip(words, (v[:1] for v in halves(e[:, at], e[:, at]))))
        for chip in chips:
            for k in reversed(range(CORES)):
                to = chip * CORES + k
                up_row = (0, *divmod((to + 1) % nrow, CORES))
                down_row = (0, *divmod((to - 1) % nrow, CORES))
                for i, key in enumerate(((0, chip, k), up_row, down_row, (1, chip, k), (-1, chip, k))):
                    words, e = groups[place[key]]
                    sets[to, i * quarter:(i + 1) * quarter] = words
                    sets[to, 5 * quarter + i:5 * quarter + i + 1] = e

                @pl.when(r != to)
                def _():
                    send(5, sets.at[to], row2.at[r], (to, c))
    row2[r] = sets[r]
    arrived(5, row2, nrow - 1)
    picks = []
    for k in range(5):
        words = tree_sum([row2[i, k * quarter:(k + 1) * quarter] for i in range(nrow)])
        at = 5 * quarter + k
        scale = scale_from(tree_sum([row2[i, at:at + 1] for i in range(nrow)]))
        picks.append([v * scale for v in from_words(words)])
    picks.append([jnp.zeros_like(picks[0][0])] * 2)
    columns = []
    for p in range(3):
        a, b = picks[2 * p], picks[2 * p + 1]
        columns.append(jnp.concatenate(
            [jnp.where(low, a[i], half_roll(b[i])) for i in range(2)]
            + [jnp.where(low, half_roll(a[i]), b[i]) for i in range(2)], axis=0))
    picked = jnp.concatenate(split(jnp.concatenate(columns, axis=1)), axis=0)
    inner = matmul(jnp.concatenate([picked, picked], axis=1), wide[...], NN)
    out_ref[...] = out_ref[...] + inner[:rhs] + inner[rhs:]

    drained(col1, ncol - 1)
    drained(row1.at[0], nrow - 1)
    drained(row1.at[1], nrow - 1)
    drained(received, ncol - 1)
    drained(col2, ncol - 1)
    drained(row2, nrow - 1)
    for d in range(4):
        @pl.when(exists[d])
        def _():
            halo(d).wait_send()

        @pl.when(exists[opposite[d]])
        def _():
            lend(d).wait_send()


def shards(nrow, ncol, residuals, intersect_blocks, local_inverse, coarse_basis, coarse_slots, coarse_inverse):
    own, rhs = residuals.shape
    loc, nev = coarse_basis.shape
    rows, width = coarse_inverse.shape
    total = coarse_slots.shape[0]
    assert 2 * nev == LANES and rows == ncol * nev and width == nrow * nev and loc == own + 4 * BLK and own % BLK == 0
    vmem = pl.BlockSpec(memory_space=pltpu.VMEM)
    hbm = pl.BlockSpec(memory_space=pl.ANY)
    dma = pltpu.SemaphoreType.DMA
    out = pl.pallas_call(
        functools.partial(kernel, nrow, ncol),
        name="schwarz",
        out_shape=pltpu.VMEM((rhs, own), F32),
        in_specs=[hbm] * 6,
        out_specs=vmem,
        scratch_shapes=[
            pltpu.VMEM((rhs, own), BF16),
            pltpu.SMEM(intersect_blocks.shape, jnp.int32),
            pltpu.VMEM((1, total), jnp.int32),
            pltpu.VMEM((4, rhs, BLK), BF16),
            pltpu.VMEM((4, rhs, BLK), BF16),
            pltpu.VMEM((own, loc), BF16),
            pltpu.VMEM((nev, loc), F32),
            pltpu.VMEM((2 * nev, loc), BF16),
            pltpu.VMEM((loc - own, 2 * nev), BF16),
            pltpu.VMEM((rows, width), F32),
            pltpu.VMEM((2 * width, rows), BF16),
            pltpu.VMEM((rows, width), BF16),
            pltpu.VMEM((rows, 3 * width), BF16),
            pltpu.VMEM((ncol, rhs // 4 + 1, LANES), jnp.int32),
            pltpu.VMEM((2, nrow, width // 2 // LANES * (rhs // 2 + 1), LANES), jnp.int32),
            pltpu.VMEM((rhs, rows), F32),
            pltpu.VMEM((ncol, rhs // 4 + 1, LANES), jnp.int32),
            pltpu.VMEM((ncol, rhs // 4 + 1, LANES), jnp.int32),
            pltpu.VMEM((ncol, rhs // 4 + 1, LANES), jnp.int32),
            pltpu.VMEM((nrow, 5 * (rhs // 4 + 1), LANES), jnp.int32),
            pltpu.VMEM((nrow, 5 * (rhs // 4 + 1), LANES), jnp.int32),
            pltpu.VMEM((4, nev, BLK), F32),
            pltpu.VMEM((12 * nev, own), BF16),
            dma((6,)),
            dma((1,)),
            dma((4,)),
            dma((4,)),
            dma((6,)),
            pltpu.SemaphoreType.REGULAR((2,)),
        ],
        compiler_params=pltpu.CompilerParams(collective_id=0, has_side_effects=True),
    )(
        residuals.T,
        intersect_blocks,
        local_inverse,
        coarse_basis.T,
        coarse_slots.reshape(1, total),
        coarse_inverse,
    )
    return out.T


def solution(mesh):
    placed = (
        P(("row", "col"), None),
        P(("row", "col"), None),
        P(("row", "col"), None),
        P(("row", "col"), None),
        P(),
        P("row", "col"),
    )
    return jax.shard_map(
        functools.partial(shards, mesh.shape["row"], mesh.shape["col"]),
        mesh=mesh, in_specs=placed, out_specs=P(("row", "col"), None), check_vma=False,
    )
```
